64 devices in a mesh: dp: 4 (over x, y), cp: 16 (over z, core).
Axes of the slice: x: 2, y: 2, z: 8, core: 2. Of those that a mesh axis runs over, the one named last changes fastest.
The devices are a block of a 4x4x8 slice.
Arguments:
- x_in: bfloat16 [8192, 5120], P(('dp', 'cp')), parts along dimension 0
- d_y: bfloat16 [8192, 5120], P(('dp', 'cp')), parts along dimension 0
- w_q: bfloat16 [5120, 32, 128], replicated
- w_k: bfloat16 [5120, 8, 128], replicated
- w_v: bfloat16 [5120, 8, 128], replicated
- w_o: bfloat16 [32, 128, 5120], replicated
Outputs:
- output: bfloat16 [8192, 5120], P(('dp', 'cp')), parts along dimension 0
There are 4 independent parts. The reference program is written for one: setup_inputs(seed, part) draws one part's arguments, and reference() takes and returns one part's arrays. A program takes and returns all parts, laid end to end along the dimension named above; an argument that names none is the same for every part.
All inputs are finite; a program needn't handle non-finite values.
Results may differ from the reference program's by a relative error of at most 0.0114179.
Values are sent between devices in bfloat16 or wider.
A program may use at most 768 MiB of HBM per device.

```python
import jax
import jax.numpy as jnp
from jax import lax

D_MODEL = 5120
Q_HEADS = 32
KV_HEADS = 8
HEAD_DIM = 128
TOK_DEV = 128
CP_SIZE = 16
ROW_BLOCK = 32
SEQ_LEN = CP_SIZE * TOK_DEV
SEG_LEN = TOK_DEV // 2
Q_GROUP = Q_HEADS // KV_HEADS
SCORE_SCALE = HEAD_DIM ** -0.5
DY_SCALE = (SEQ_LEN / 16) ** 0.5


def token_positions(row_ids):
    dev_idx = row_ids // TOK_DEV
    row_off = row_ids % TOK_DEV
    seg_idx = jnp.where(row_off < SEG_LEN, dev_idx, 2 * CP_SIZE - 1 - dev_idx)
    return seg_idx * SEG_LEN + row_off % SEG_LEN


def setup_inputs(seed: int = 0, part: int = 0) -> dict:
    part_key = jax.random.fold_in(jax.random.key(seed), part)
    key_x, key_dy = jax.random.split(part_key)
    key_q, key_k, key_v, key_o = jax.random.split(jax.random.key(seed + 1), 4)
    x_in = jax.random.normal(key_x, (SEQ_LEN, D_MODEL), jnp.float32).astype(jnp.bfloat16)
    d_y = (jax.random.normal(key_dy, (SEQ_LEN, D_MODEL), jnp.float32) * DY_SCALE).astype(jnp.bfloat16)
    w_q = (jax.random.normal(key_q, (D_MODEL, Q_HEADS, HEAD_DIM), jnp.float32) * D_MODEL ** -0.5).astype(jnp.bfloat16)
    w_k = (jax.random.normal(key_k, (D_MODEL, KV_HEADS, HEAD_DIM), jnp.float32) * D_MODEL ** -0.5).astype(jnp.bfloat16)
    w_v = (jax.random.normal(key_v, (D_MODEL, KV_HEADS, HEAD_DIM), jnp.float32) * D_MODEL ** -0.5).astype(jnp.bfloat16)
    w_o = (jax.random.normal(key_o, (Q_HEADS, HEAD_DIM, D_MODEL), jnp.float32) * (Q_HEADS * HEAD_DIM) ** -0.5).astype(jnp.bfloat16)
    return {"x_in": x_in, "d_y": d_y, "w_q": w_q, "w_k": w_k, "w_v": w_v, "w_o": w_o}


def reference(x_in, d_y, w_q, w_k, w_v, w_o):
    wq_flat = w_q.reshape(D_MODEL, Q_HEADS * HEAD_DIM)
    wk_flat = w_k.reshape(D_MODEL, KV_HEADS * HEAD_DIM)
    wv_flat = w_v.reshape(D_MODEL, KV_HEADS * HEAD_DIM)
    wo_flat = w_o.reshape(Q_HEADS * HEAD_DIM, D_MODEL)
    q_proj = jnp.dot(x_in, wq_flat, preferred_element_type=jnp.float32).astype(jnp.bfloat16)
    k_proj = jnp.dot(x_in, wk_flat, preferred_element_type=jnp.float32).astype(jnp.bfloat16)
    v_proj = jnp.dot(x_in, wv_flat, preferred_element_type=jnp.float32).astype(jnp.bfloat16)
    do_proj = jnp.dot(d_y, wo_flat.T, preferred_element_type=jnp.float32).astype(jnp.bfloat16)
    queries = q_proj.astype(jnp.float32).reshape(SEQ_LEN, KV_HEADS, Q_GROUP, HEAD_DIM)
    key_all = k_proj.astype(jnp.float32).reshape(SEQ_LEN, KV_HEADS, HEAD_DIM)
    val_all = v_proj.astype(jnp.float32).reshape(SEQ_LEN, KV_HEADS, HEAD_DIM)
    d_out = do_proj.astype(jnp.float32).reshape(SEQ_LEN, KV_HEADS, Q_GROUP, HEAD_DIM)
    positions = token_positions(jnp.arange(SEQ_LEN))

    def block_step(acc_pair, blk_idx):
        dk_acc, dv_acc = acc_pair
        row_start = blk_idx * ROW_BLOCK
        q_blk = lax.dynamic_slice_in_dim(queries, row_start, ROW_BLOCK, 0)
        do_blk = lax.dynamic_slice_in_dim(d_out, row_start, ROW_BLOCK, 0)
        pos_blk = lax.dynamic_slice_in_dim(positions, row_start, ROW_BLOCK, 0)
        scores = jnp.einsum("rkge,ske->krgs", q_blk, key_all) * SCORE_SCALE
        causal = pos_blk[None, :, None, None] >= positions[None, None, None, :]
        scores = jnp.where(causal, scores, -jnp.inf)
        lse_blk = jax.nn.logsumexp(scores, axis=-1, keepdims=True)
        prob_blk = jnp.exp(scores - lse_blk).astype(jnp.bfloat16).astype(jnp.float32)
        out_blk = jnp.einsum("krgs,ske->krge", prob_blk, val_all).astype(jnp.bfloat16).astype(jnp.float32)
        row_delta = jnp.einsum("rkge,krge->krg", do_blk, out_blk)
        dp_blk = jnp.einsum("rkge,ske->krgs", do_blk, val_all)
        ds_blk = (prob_blk * (dp_blk - row_delta[..., None])).astype(jnp.bfloat16).astype(jnp.float32)
        dq_blk = (jnp.einsum("krgs,ske->rkge", ds_blk, key_all) * SCORE_SCALE).astype(jnp.bfloat16)
        dk_acc = dk_acc + jnp.einsum("krgs,rkge->ske", ds_blk, q_blk)
        dv_acc = dv_acc + jnp.einsum("krgs,rkge->ske", prob_blk, do_blk)
        return (dk_acc, dv_acc), dq_blk

    zero_acc = jnp.zeros((SEQ_LEN, KV_HEADS, HEAD_DIM), jnp.float32)
    (dk_sum, dv_sum), dq_blocks = lax.scan(block_step, (zero_acc, zero_acc), jnp.arange(SEQ_LEN // ROW_BLOCK))
    d_query = dq_blocks.reshape(SEQ_LEN, Q_HEADS * HEAD_DIM)
    d_key = (dk_sum * SCORE_SCALE).astype(jnp.bfloat16).reshape(SEQ_LEN, KV_HEADS * HEAD_DIM)
    d_value = dv_sum.astype(jnp.bfloat16).reshape(SEQ_LEN, KV_HEADS * HEAD_DIM)
    d_x = jnp.dot(d_query, wq_flat.T, preferred_element_type=jnp.float32)
    d_x = d_x + jnp.dot(d_key, wk_flat.T, preferred_element_type=jnp.float32)
    d_x = d_x + jnp.dot(d_value, wv_flat.T, preferred_element_type=jnp.float32)
    return d_x.astype(jnp.bfloat16)
```

```python
import functools

import jax
import jax.numpy as jnp
from jax import lax
from jax.experimental import pallas as pl
from jax.experimental.pallas import tpu as pltpu
from jax.sharding import PartitionSpec as P

MESH = pl.DeviceIdType.MESH
BF16 = jnp.bfloat16
F32 = jnp.float32
CONTRACT_LAST = (((1,), (1,)), ((), ()))
DEPTH = 4
WO_DEPTH = 3
D_CHUNK = 512
VMEM_LIMIT = 62 * 2 ** 20


def place():
    me = lax.axis_index("cp")
    chip = me // 2
    core = me % 2
    return me, chip, core, me + 1 - 2 * core


def meet_group(n_dev):
    me = lax.axis_index("cp")
    barrier = pltpu.get_barrier_semaphore()

    def greet(step, carry):
        other = lax.rem(me + step, n_dev)
        pl.semaphore_signal(barrier, inc=1, device_id={"cp": other}, device_id_type=MESH)
        return carry

    lax.fori_loop(1, n_dev, greet, 0)
    pl.semaphore_wait(barrier, n_dev - 1)


def rcopy(src, dst, send_sem, recv_sem, dev):
    return pltpu.make_async_remote_copy(
        src_ref=src, dst_ref=dst, send_sem=send_sem, recv_sem=recv_sem,
        device_id={"cp": dev}, device_id_type=MESH)


def al(value, step):
    return pl.multiple_of(value, step)


def ship_start(is_me, src, dst, send_sem, recv_sem, dev):
    @pl.when(is_me)
    def _():
        pltpu.make_async_copy(src, dst, send_sem).start()

    @pl.when(jnp.logical_not(is_me))
    def _():
        rcopy(src, dst, send_sem, recv_sem, dev).start()


def ship_wait(is_me, src, dst, send_sem, recv_sem, dev):
    @pl.when(is_me)
    def _():
        pltpu.make_async_copy(src, dst, send_sem).wait()

    @pl.when(jnp.logical_not(is_me))
    def _():
        rcopy(src, dst, send_sem, recv_sem, dev).wait_send()


def project_kernel(n_dev, x_ref, dy_ref, wq, wk, wv, wo, q_all, do_all, kv_all,
                   xs, dys, wo_buf, w_buf, acc, st_do, st_kv, st_q,
                   wo_sem, w_sem, x_send, x_recv, do_send, do_recv,
                   kv_send, kv_recv, q_send, q_recv, rel_send, rel_recv):
    me, chip, core, sib = place()
    n_chip = n_dev // 2
    rows, d_model = x_ref.shape
    seg = rows // 2
    head = kv_all.shape[2]
    wide = q_all.shape[1]
    tile_w = acc.shape[1]
    n_chunk = d_model // D_CHUNK
    n_dest = n_dev // 2
    tile_heads = w_buf.shape[2]
    my_src_core = chip // (n_chip // 2)
    low_at = al(chip * rows, rows)
    high_at = al((2 * n_chip - 1 - chip) * rows, rows)

    def dest_of(n):
        return n_dest * core + lax.rem(n + 2 * chip, n_dest)

    def wo_copy(n):
        return pltpu.make_async_copy(
            wo.at[pl.ds(al(dest_of(n) * wide, wide), wide), :], wo_buf.at[lax.rem(n, WO_DEPTH)],
            wo_sem.at[lax.rem(n, WO_DEPTH)])

    def tile_of(t):
        return 2 * core + lax.rem(t + chip // 2, 2)

    def w_start(s):
        slot = lax.rem(s, DEPTH)
        part = lax.rem(s, n_chunk)
        d_rows = pl.ds(al(part * D_CHUNK, D_CHUNK), D_CHUNK)

        @pl.when((s < n_chunk) & (core == 0))
        def _():
            pltpu.make_async_copy(wk.at[d_rows], w_buf.at[slot], w_sem.at[slot]).start()

        @pl.when((s < n_chunk) & (core == 1))
        def _():
            pltpu.make_async_copy(wv.at[d_rows], w_buf.at[slot], w_sem.at[slot]).start()

        @pl.when((s >= n_chunk) & (s < 3 * n_chunk))
        def _():
            tile = tile_of(s // n_chunk - 1)
            pltpu.make_async_copy(
                wq.at[d_rows, pl.ds(al(tile * tile_heads, tile_heads), tile_heads), :],
                w_buf.at[slot], w_sem.at[slot]).start()

    def w_wait(s):
        slot = lax.rem(s, DEPTH)
        pltpu.make_async_copy(wk.at[pl.ds(0, D_CHUNK)], w_buf.at[slot], w_sem.at[slot]).wait()

    for n in range(WO_DEPTH - 1):
        wo_copy(n).start()
    for s in range(DEPTH - 1):
        w_start(s)

    my_low = al(core * seg, seg)
    my_high = al(rows + (1 - core) * seg, seg)
    for ref, stack in ((dy_ref, dys), (x_ref, xs)):
        stack[pl.ds(my_low, seg), :] = ref[:seg, :]
        stack[pl.ds(my_high, seg), :] = ref[seg:, :]
    meet_group(n_dev)
    swaps = []
    for k, (ref, stack) in enumerate(((dy_ref, dys), (x_ref, xs))):
        swaps.append(rcopy(ref.at[pl.ds(0, seg)], stack.at[pl.ds(my_low, seg)],
                           x_send.at[k, 0], x_recv.at[k, 0], sib))
        swaps.append(rcopy(ref.at[pl.ds(seg, seg)], stack.at[pl.ds(my_high, seg)],
                           x_send.at[k, 1], x_recv.at[k, 1], sib))
    for swap in swaps:
        swap.start()
    swaps[0].wait()
    swaps[1].wait()

    def do_ship(n, act):
        dest = dest_of(n)
        for k, at in enumerate((low_at, high_at)):
            act(dest == me, st_do.at[n, pl.ds(k * rows, rows), :], do_all.at[pl.ds(at, rows), :],
                do_send.at[n, k], do_recv.at[chip, k], dest)

    def do_step(n, carry):
        @pl.when(n + WO_DEPTH - 1 < n_dest)
        def _():
            wo_copy(n + WO_DEPTH - 1).start()
        wo_copy(n).wait()

        @pl.when(n > 0)
        def _():
            do_ship(n - 1, ship_start)
        st_do[n] = lax.dot_general(dys[...], wo_buf[lax.rem(n, WO_DEPTH)], CONTRACT_LAST,
                                   preferred_element_type=F32).astype(BF16)
        return carry

    lax.fori_loop(0, n_dest, do_step, 0)
    swaps[2].wait()
    swaps[3].wait()

    def w_step(s, first):
        w_start(s + DEPTH - 1)
        w_wait(s)
        part = lax.rem(s, n_chunk)
        w_tile = w_buf[lax.rem(s, DEPTH)].reshape(D_CHUNK, tile_w)
        add = jnp.dot(xs[:, pl.ds(al(part * D_CHUNK, D_CHUNK), D_CHUNK)], w_tile,
                      preferred_element_type=F32)
        acc[...] = add if first else acc[...] + add

    def w_loop(lo, hi):
        def body(s, carry):
            w_step(s, False)
            return carry
        lax.fori_loop(lo, hi, body, 0)

    def kv_ship(dest_chip, act):
        dest = 2 * dest_chip + core
        lanes = pl.ds(al(dest_chip * head, head), head)
        for k, at in enumerate((low_at, high_at)):
            act(dest == me, st_kv.at[pl.ds(k * rows, rows), lanes], kv_all.at[core, pl.ds(at, rows), :],
                kv_send.at[dest_chip, k], kv_recv.at[chip, k], dest)

    def kv_ship_all(act):
        def body(n, carry):
            kv_ship(lax.rem(n + chip, n_chip), act)
            return carry
        lax.fori_loop(0, n_chip, body, 0)

    def q_ship(t, n, act):
        dest = 4 * tile_of(t) + lax.rem(n + 2 * chip, 4)
        lanes = pl.ds(al(lax.rem(dest, 4) * wide, wide), wide)
        for k, at in enumerate((low_at, high_at)):
            act(dest == me, st_q.at[t, pl.ds(k * rows, rows), lanes], q_all.at[pl.ds(at, rows), :],
                q_send.at[4 * t + n, k], q_recv.at[chip, k], dest)

    def q_ship_all(t, act):
        def body(n, carry):
            q_ship(t, n, act)
            return carry
        lax.fori_loop(0, 4, body, 0)

    w_step(0, True)
    do_ship(n_dest - 1, ship_start)
    w_loop(1, n_chunk)
    st_kv[...] = acc[...].astype(BF16)
    w_step(n_chunk, True)
    kv_ship_all(ship_start)
    w_loop(n_chunk + 1, 2 * n_chunk)
    st_q[0] = acc[...].astype(BF16)
    w_step(2 * n_chunk, True)
    q_ship_all(0, ship_start)
    w_loop(2 * n_chunk + 1, 3 * n_chunk)
    st_q[1] = acc[...].astype(BF16)

    def kv_arrive(src_chip, carry):
        @pl.when(src_chip != chip)
        def _():
            for k in range(2):
                rcopy(st_kv.at[pl.ds(0, rows), pl.ds(0, head)], kv_all.at[core, pl.ds(0, rows), :],
                      kv_send.at[0, k], kv_recv.at[src_chip, k], sib).wait_recv()
        return carry

    lax.fori_loop(0, n_chip, kv_arrive, 0)
    q_ship_all(1, ship_start)
    kv_ship_all(ship_wait)
    relay = rcopy(kv_all.at[core], kv_all.at[core], rel_send, rel_recv, sib)
    relay.start()

    def wide_arrive(src_chip, carry):
        @pl.when(2 * src_chip + my_src_core != me)
        def _():
            for k in range(2):
                rcopy(st_do.at[0, pl.ds(0, rows), :], do_all.at[pl.ds(0, rows), :],
                      do_send.at[0, k], do_recv.at[src_chip, k], sib).wait_recv()
                rcopy(st_do.at[0, pl.ds(0, rows), :], q_all.at[pl.ds(0, rows), :],
                      q_send.at[0, k], q_recv.at[src_chip, k], sib).wait_recv()
        return carry

    lax.fori_loop(0, n_chip, wide_arrive, 0)

    def do_done(n, carry):
        do_ship(n, ship_wait)
        return carry

    lax.fori_loop(0, n_dest, do_done, 0)
    q_ship_all(0, ship_wait)
    q_ship_all(1, ship_wait)
    rcopy(kv_all.at[core], kv_all.at[1 - core], rel_send, rel_recv, sib).wait_recv()
    relay.wait_send()


def attend_kernel(scale, q_ref, do_ref, kv_ref, dq_ref, dkv_ref, k_t, v_t, s_scr, p_scr):
    seq, wide = q_ref.shape
    head = kv_ref.shape[2]
    heads = wide // head
    bq, bk = 256, 512
    k_t[...] = kv_ref[0].T
    v_t[...] = kv_ref[1].T
    dkv_ref[...] = jnp.zeros_like(dkv_ref)
    to_log2 = scale * 1.4426950408889634

    def q_block(qb, carry):
        q_rows = pl.ds(al(qb * bq, bq), bq)
        q = [q_ref[q_rows, h * head:(h + 1) * head] for h in range(heads)]
        do = [do_ref[q_rows, h * head:(h + 1) * head] for h in range(heads)]
        last = (qb * bq) // bk

        def keys(kc):
            return pl.ds(al(kc * bk, bk), bk)

        def scores(kc, tops, masked):
            k_blk = kv_ref[0, keys(kc), :]
            out = []
            for h in range(heads):
                s = lax.dot_general(k_blk, q[h], CONTRACT_LAST, preferred_element_type=F32)
                if masked:
                    k_pos = kc * bk + lax.broadcasted_iota(jnp.int32, (bk, bq), 0)
                    q_pos = qb * bq + lax.broadcasted_iota(jnp.int32, (bk, bq), 1)
                    s = jnp.where(k_pos <= q_pos, s, -jnp.inf)
                s_scr[h, keys(kc), :] = s
                out.append(jnp.maximum(tops[h], jnp.max(s, axis=0, keepdims=True)))
            return tuple(out)

        tops = tuple(jnp.full((1, bq), -jnp.inf, F32) for _ in range(heads))
        tops = lax.fori_loop(0, last, lambda kc, c: scores(kc, c, False), tops)
        tops = scores(last, tops, True)
        tops = [t * to_log2 for t in tops]

        def expo(kc, sums):
            out = []
            for h in range(heads):
                e = jnp.exp2(s_scr[h, keys(kc), :] * to_log2 - tops[h])
                s_scr[h, keys(kc), :] = e
                out.append(sums[h] + jnp.sum(e, axis=0, keepdims=True))
            return tuple(out)

        sums = lax.fori_loop(0, last + 1, expo, tuple(jnp.zeros((1, bq), F32) for _ in range(heads)))
        inv = [1.0 / s for s in sums]

        def outs(kc, acc):
            v_blk = v_t[:, keys(kc)]
            out = []
            for h in range(heads):
                p = (s_scr[h, keys(kc), :] * inv[h]).astype(BF16)
                p_scr[h, keys(kc), :] = p
                out.append(acc[h] + jnp.dot(v_blk, p, preferred_element_type=F32))
            return tuple(out)

        zero = tuple(jnp.zeros((head, bq), F32) for _ in range(heads))
        o_t = lax.fori_loop(0, last + 1, outs, zero)
        delta = [jnp.sum(do[h].astype(F32).T * o_t[h].astype(BF16).astype(F32), axis=0, keepdims=True)
                 for h in range(heads)]

        def grads(kc, acc):
            k_blk = k_t[:, keys(kc)]
            v_blk = kv_ref[1, keys(kc), :]
            out = []
            dk = dv = None
            for h in range(heads):
                p = p_scr[h, keys(kc), :]
                dp = lax.dot_general(v_blk, do[h], CONTRACT_LAST, preferred_element_type=F32)
                ds = (p.astype(F32) * (dp - delta[h])).astype(BF16)
                out.append(acc[h] + jnp.dot(k_blk, ds, preferred_element_type=F32))
                dk_h = jnp.dot(ds, q[h], preferred_element_type=F32)
                dv_h = jnp.dot(p, do[h], preferred_element_type=F32)
                dk = dk_h if dk is None else dk + dk_h
                dv = dv_h if dv is None else dv + dv_h
            dkv_ref[0, keys(kc), :] += dk
            dkv_ref[1, keys(kc), :] += dv
            return tuple(out)

        dq_t = lax.fori_loop(0, last + 1, grads, zero)
        for h in range(heads):
            dq_ref[q_rows, h * head:(h + 1) * head] = (dq_t[h] * scale).T.astype(BF16)
        return carry

    lax.fori_loop(0, seq // bq, q_block, 0)


def collect_kernel(n_dev, scale, dq_ref, dkv_ref, wq, wk, wv, dx_ref,
                   dq_in, dkv_in, dkv_far, dkv_st, w_buf, w2, acc, far,
                   w_sem, dq_send, dq_recv, dkv_send, dkv_recv, far_send, far_recv, red_send, red_recv):
    me, chip, core, sib = place()
    n_chip = n_dev // 2
    rows, d_model = dx_ref.shape
    seg = rows // 2
    head = dkv_ref.shape[2]
    wide = dq_ref.shape[1]
    n_chunk = d_model // D_CHUNK
    tile_heads = w_buf.shape[2]
    tile_w = w2.shape[2]
    half_dev = n_dev // 2
    dq_core = chip // (n_chip // 2)

    def w_start(s):
        slot = lax.rem(s, DEPTH)
        part = lax.rem(s, n_chunk)
        d_rows = pl.ds(al(part * D_CHUNK, D_CHUNK), D_CHUNK)

        @pl.when(s < 2 * n_chunk)
        def _():
            tile = 2 * core + s // n_chunk
            pltpu.make_async_copy(
                wq.at[d_rows, pl.ds(al(tile * tile_heads, tile_heads), tile_heads), :],
                w_buf.at[slot], w_sem.at[slot]).start()

        @pl.when((s >= 2 * n_chunk) & (s < 3 * n_chunk) & (core == 0))
        def _():
            pltpu.make_async_copy(wk.at[d_rows], w_buf.at[slot], w_sem.at[slot]).start()

        @pl.when((s >= 2 * n_chunk) & (s < 3 * n_chunk) & (core == 1))
        def _():
            pltpu.make_async_copy(wv.at[d_rows], w_buf.at[slot], w_sem.at[slot]).start()

    for s in range(DEPTH - 1):
        w_start(s)
    meet_group(n_dev)
    swap = rcopy(dkv_ref.at[1 - core], dkv_far, red_send, red_recv, sib)
    swap.start()

    src_slot = lax.rem(me, half_dev)

    def at_of(dest_chip, k):
        block = dest_chip if k == 0 else 2 * n_chip - 1 - dest_chip
        return al(block * rows, rows)

    def dq_ship(n, act):
        dest_chip = lax.rem(chip + n, n_chip)
        dest = 2 * dest_chip + dq_core
        for k in range(2):
            act(dest == me, dq_ref.at[pl.ds(at_of(dest_chip, k), rows), :],
                dq_in.at[src_slot // 4, pl.ds(k * rows, rows), pl.ds(al(lax.rem(src_slot, 4) * wide, wide), wide)],
                dq_send.at[n, k], dq_recv.at[src_slot, k], dest)

    def dkv_ship(n, act):
        dest_chip = lax.rem(chip + n, n_chip)
        dest = 2 * dest_chip + core
        for k in range(2):
            act(dest == me, dkv_st.at[pl.ds(at_of(dest_chip, k), rows), :],
                dkv_in.at[pl.ds(k * rows, rows), pl.ds(al(chip * head, head), head)],
                dkv_send.at[n, k], dkv_recv.at[chip, k], dest)

    def each(ship, act):
        def body(n, carry):
            ship(n, act)
            return carry
        lax.fori_loop(0, n_chip, body, 0)

    each(dq_ship, ship_start)
    swap.wait()
    factor = jnp.where(core == 0, scale, 1.0).astype(F32)
    dkv_st[...] = ((dkv_ref[core] + dkv_far[...]) * factor).astype(BF16)

    def turn(s, carry):
        w_start(s + DEPTH - 1)
        slot = lax.rem(s, DEPTH)
        pltpu.make_async_copy(wk.at[pl.ds(0, D_CHUNK)], w_buf.at[slot], w_sem.at[slot]).wait()
        w2[s] = w_buf[slot].reshape(D_CHUNK, tile_w)
        return carry

    turn(0, 0)
    each(dkv_ship, ship_start)
    lax.fori_loop(1, 3 * n_chunk, turn, 0)

    def dq_arrive(src, carry):
        @pl.when(half_dev * core + src != me)
        def _():
            pass
        return carry

    def arrive_dq(lo, hi):
        def body(src, carry):
            @pl.when((half_dev * core + src != me))
            def _():
                for k in range(2):
                    rcopy(dq_ref.at[pl.ds(0, rows), :],
                          dq_in.at[0, pl.ds(0, rows), pl.ds(0, wide)],
                          dq_send.at[0, k], dq_recv.at[src, k], sib).wait_recv()
            return carry
        lax.fori_loop(lo, hi, body, 0)

    def matmul(act, base, part):
        return lax.dot_general(act, w2[base + part], CONTRACT_LAST, preferred_element_type=F32)

    each(dq_ship, ship_wait)
    arrive_dq(0, half_dev)

    def first_pass(part, carry):
        acc[part] = matmul(dq_in[0], 0, part) + matmul(dq_in[1], n_chunk, part)
        return carry

    lax.fori_loop(0, n_chunk, first_pass, 0)

    each(dkv_ship, ship_wait)

    def dkv_arrive(src_chip, carry):
        @pl.when(src_chip != chip)
        def _():
            for k in range(2):
                rcopy(dkv_st.at[pl.ds(0, rows), :], dkv_in.at[pl.ds(0, rows), pl.ds(0, head)],
                      dkv_send.at[0, k], dkv_recv.at[src_chip, k], sib).wait_recv()
        return carry

    lax.fori_loop(0, n_chip, dkv_arrive, 0)

    sib_low = al((1 - core) * seg, seg)
    sib_high = al(rows + core * seg, seg)
    my_low = al(core * seg, seg)
    my_high = al(rows + (1 - core) * seg, seg)

    def far_copy(part, k):
        src_at = sib_low if k == 0 else sib_high
        return rcopy(acc.at[part, pl.ds(src_at, seg), :], far.at[part, pl.ds(k * seg, seg), :],
                     far_send.at[part, k], far_recv.at[part, k], sib)

    def last_pass(part, carry):
        acc[part] += matmul(dkv_in[...], 2 * n_chunk, part)

        @pl.when(part > 0)
        def _():
            for k in range(2):
                far_copy(part - 1, k).start()
        return carry

    lax.fori_loop(0, n_chunk, last_pass, 0)
    for k in range(2):
        far_copy(n_chunk - 1, k).start()

    def finish(part, carry):
        for k in range(2):
            far_copy(part, k).wait()
        lanes = pl.ds(al(part * D_CHUNK, D_CHUNK), D_CHUNK)
        dx_ref[pl.ds(0, seg), lanes] = (acc[part, pl.ds(my_low, seg), :] + far[part, pl.ds(0, seg), :]).astype(BF16)
        dx_ref[pl.ds(seg, seg), lanes] = (acc[part, pl.ds(my_high, seg), :] + far[part, pl.ds(seg, seg), :]).astype(BF16)
        return carry

    lax.fori_loop(0, n_chunk, finish, 0)


def solution(mesh):
    n_dev = mesh.shape["cp"]
    n_chip = n_dev // 2
    row_spec = P(("dp", "cp"), None)
    any_spec = pl.BlockSpec(memory_space=pl.ANY)
    vmem_spec = pl.BlockSpec(memory_space=pltpu.VMEM)
    dma = pltpu.SemaphoreType.DMA

    def device_fn(x_in, d_y, w_q, w_k, w_v, w_o):
        rows, d_model = x_in.shape
        q_heads, head = w_q.shape[1], w_q.shape[2]
        kv_heads = w_k.shape[1]
        seq = rows * n_dev
        scale = head ** -0.5
        wide = q_heads // n_dev * head
        tile_w = kv_heads * head
        n_chunk = d_model // D_CHUNK
        wo_flat = w_o.reshape(q_heads * head, d_model)
        params = functools.partial(pltpu.CompilerParams, vmem_limit_bytes=VMEM_LIMIT)
        q_all, do_all, kv_all = pl.pallas_call(
            functools.partial(project_kernel, n_dev),
            out_shape=(jax.ShapeDtypeStruct((seq, wide), BF16),
                       jax.ShapeDtypeStruct((seq, wide), BF16),
                       jax.ShapeDtypeStruct((2, seq, head), BF16)),
            in_specs=[vmem_spec, vmem_spec, any_spec, any_spec, any_spec, any_spec],
            out_specs=[any_spec] * 3,
            scratch_shapes=[
                pltpu.VMEM((2 * rows, d_model), BF16),
                pltpu.VMEM((2 * rows, d_model), BF16),
                pltpu.VMEM((WO_DEPTH, wide, d_model), BF16),
                pltpu.VMEM((DEPTH, D_CHUNK, kv_heads, head), BF16),
                pltpu.VMEM((2 * rows, tile_w), F32),
                pltpu.VMEM((n_chip, 2 * rows, wide), BF16),
                pltpu.VMEM((2 * rows, tile_w), BF16),
                pltpu.VMEM((2, 2 * rows, tile_w), BF16),
                dma((WO_DEPTH,)), dma((DEPTH,)), dma((2, 2)), dma((2, 2)),
                dma((n_chip, 2)), dma((n_chip, 2)), dma((n_chip, 2)), dma((n_chip, 2)),
                dma((n_chip, 2)), dma((n_chip, 2)), dma, dma,
            ],
            compiler_params=params(collective_id=0, has_side_effects=True),
            name="project",
        )(x_in, d_y, w_q, w_k, w_v, wo_flat)
        dq_all, dkv_part = pl.pallas_call(
            functools.partial(attend_kernel, scale),
            out_shape=(jax.ShapeDtypeStruct((seq, wide), BF16),
                       jax.ShapeDtypeStruct((2, seq, head), F32)),
            in_specs=[vmem_spec] * 3,
            out_specs=[vmem_spec] * 2,
            scratch_shapes=[
                pltpu.VMEM((head, seq), BF16),
                pltpu.VMEM((head, seq), BF16),
                pltpu.VMEM((wide // head, seq, 256), F32),
                pltpu.VMEM((wide // head, seq, 256), BF16),
            ],
            compiler_params=params(),
            name="attend",
        )(q_all, do_all, kv_all)
        return pl.pallas_call(
            functools.partial(collect_kernel, n_dev, scale),
            out_shape=jax.ShapeDtypeStruct((rows, d_model), BF16),
            in_specs=[vmem_spec, vmem_spec, any_spec, any_spec, any_spec],
            out_specs=vmem_spec,
            scratch_shapes=[
                pltpu.VMEM((2, 2 * rows, tile_w), BF16),
                pltpu.VMEM((2 * rows, tile_w), BF16),
                pltpu.VMEM((seq, head), F32),
                pltpu.VMEM((seq, head), BF16),
                pltpu.VMEM((DEPTH, D_CHUNK, kv_heads, head), BF16),
                pltpu.VMEM((3 * n_chunk, D_CHUNK, tile_w), BF16),
                pltpu.VMEM((n_chunk, 2 * rows, D_CHUNK), F32),
                pltpu.VMEM((n_chunk, rows, D_CHUNK), F32),
                dma((DEPTH,)), dma((n_chip, 2)), dma((n_chip, 2)), dma((n_chip, 2)), dma((n_chip, 2)),
                dma((n_chunk, 2)), dma((n_chunk, 2)), dma, dma,
            ],
            compiler_params=params(collective_id=1, has_side_effects=True),
            name="collect",
        )(dq_all, dkv_part, w_q, w_k, w_v)

    return jax.shard_map(device_fn, mesh=mesh, in_specs=(row_spec, row_spec, P(), P(), P(), P()),
                         out_specs=row_spec, check_vma=False)
```

```python
import functools

import jax
import jax.numpy as jnp
from jax import lax
from jax.experimental import pallas as pl
from jax.experimental.pallas import tpu as pltpu
from jax.sharding import PartitionSpec as P

MESH = pl.DeviceIdType.MESH
BF16 = jnp.bfloat16
F32 = jnp.float32
CONTRACT_LAST = (((1,), (1,)), ((), ()))
DEPTH = 4
WO_DEPTH = 3
D_CHUNK = 512
BQ = 256
BK = 512
VMEM_LIMIT = 62 * 2 ** 20


def place():
    me = lax.axis_index("cp")
    chip = me // 2
    core = me % 2
    return me, chip, core, me + 1 - 2 * core


def meet_group(n_dev):
    me = lax.axis_index("cp")
    barrier = pltpu.get_barrier_semaphore()

    def greet(step, carry):
        other = lax.rem(me + step, n_dev)
        pl.semaphore_signal(barrier, inc=1, device_id={"cp": other}, device_id_type=MESH)
        return carry

    lax.fori_loop(1, n_dev, greet, 0)
    pl.semaphore_wait(barrier, n_dev - 1)


def rcopy(src, dst, send_sem, recv_sem, dev):
    return pltpu.make_async_remote_copy(
        src_ref=src, dst_ref=dst, send_sem=send_sem, recv_sem=recv_sem,
        device_id={"cp": dev}, device_id_type=MESH)


def al(value, step):
    return pl.multiple_of(value, step)


def ship_start(is_me, src, dst, send_sem, recv_sem, dev):
    @pl.when(is_me)
    def _():
        pltpu.make_async_copy(src, dst, send_sem).start()

    @pl.when(jnp.logical_not(is_me))
    def _():
        rcopy(src, dst, send_sem, recv_sem, dev).start()


def ship_wait(is_me, src, dst, send_sem, recv_sem, dev):
    @pl.when(is_me)
    def _():
        pltpu.make_async_copy(src, dst, send_sem).wait()

    @pl.when(jnp.logical_not(is_me))
    def _():
        rcopy(src, dst, send_sem, recv_sem, dev).wait_send()


def project_kernel(n_dev, x_ref, dy_ref, wq, wk, wv, wo, q_all, do_all, kv_all, w2_all,
                   xs, dys, wo_buf, w_buf, w2_buf, acc, st_do, st_kv, st_q,
                   wo_sem, w_sem, w2_sem, x_send, x_recv, do_send, do_recv,
                   kv_send, kv_recv, q_send, q_recv, rel_send, rel_recv):
    me, chip, core, sib = place()
    n_chip = n_dev // 2
    rows, d_model = x_ref.shape
    seg = rows // 2
    head = kv_all.shape[2]
    wide = q_all.shape[1]
    tile_w = acc.shape[1]
    n_chunk = d_model // D_CHUNK
    n_dest = n_dev // 2
    tile_heads = w_buf.shape[2]
    my_src_core = chip // (n_chip // 2)
    low_at = al(chip * rows, rows)
    high_at = al((2 * n_chip - 1 - chip) * rows, rows)

    def dest_of(n):
        return n_dest * core + lax.rem(n + 2 * chip, n_dest)

    def wo_copy(n):
        return pltpu.make_async_copy(
            wo.at[pl.ds(al(dest_of(n) * wide, wide), wide), :], wo_buf.at[lax.rem(n, WO_DEPTH)],
            wo_sem.at[lax.rem(n, WO_DEPTH)])

    def tile_of(t):
        return 2 * core + lax.rem(t + chip // 2, 2)

    def w_start(s):
        slot = lax.rem(s, DEPTH)
        part = lax.rem(s, n_chunk)
        d_rows = pl.ds(al(part * D_CHUNK, D_CHUNK), D_CHUNK)

        @pl.when((s < n_chunk) & (core == 0))
        def _():
            pltpu.make_async_copy(wk.at[d_rows], w_buf.at[slot], w_sem.at[slot]).start()

        @pl.when((s < n_chunk) & (core == 1))
        def _():
            pltpu.make_async_copy(wv.at[d_rows], w_buf.at[slot], w_sem.at[slot]).start()

        @pl.when((s >= n_chunk) & (s < 3 * n_chunk))
        def _():
            tile = tile_of(s // n_chunk - 1)
            pltpu.make_async_copy(
                wq.at[d_rows, pl.ds(al(tile * tile_heads, tile_heads), tile_heads), :],
                w_buf.at[slot], w_sem.at[slot]).start()

    def w_wait(s):
        slot = lax.rem(s, DEPTH)
        pltpu.make_async_copy(wk.at[pl.ds(0, D_CHUNK)], w_buf.at[slot], w_sem.at[slot]).wait()

    for n in range(WO_DEPTH - 1):
        wo_copy(n).start()
    for s in range(DEPTH - 1):
        w_start(s)

    my_low = al(core * seg, seg)
    my_high = al(rows + (1 - core) * seg, seg)
    for ref, stack in ((dy_ref, dys), (x_ref, xs)):
        stack[pl.ds(my_low, seg), :] = ref[:seg, :]
        stack[pl.ds(my_high, seg), :] = ref[seg:, :]
    meet_group(n_dev)
    swaps = []
    for k, (ref, stack) in enumerate(((dy_ref, dys), (x_ref, xs))):
        swaps.append(rcopy(ref.at[pl.ds(0, seg)], stack.at[pl.ds(my_low, seg)],
                           x_send.at[k, 0], x_recv.at[k, 0], sib))
        swaps.append(rcopy(ref.at[pl.ds(seg, seg)], stack.at[pl.ds(my_high, seg)],
                           x_send.at[k, 1], x_recv.at[k, 1], sib))
    for swap in swaps:
        swap.start()
    swaps[0].wait()
    swaps[1].wait()

    def do_ship(n, act):
        dest = dest_of(n)
        for k, at in enumerate((low_at, high_at)):
            act(dest == me, st_do.at[n, pl.ds(k * rows, rows), :], do_all.at[pl.ds(at, rows), :],
                do_send.at[n, k], do_recv.at[chip, k], dest)

    def do_step(n, carry):
        @pl.when(n + WO_DEPTH - 1 < n_dest)
        def _():
            wo_copy(n + WO_DEPTH - 1).start()
        wo_copy(n).wait()

        @pl.when(n > 0)
        def _():
            do_ship(n - 1, ship_start)
        st_do[n] = lax.dot_general(dys[...], wo_buf[lax.rem(n, WO_DEPTH)], CONTRACT_LAST,
                                   preferred_element_type=F32).astype(BF16)
        return carry

    lax.fori_loop(0, n_dest, do_step, 0)
    swaps[2].wait()
    swaps[3].wait()

    def w2_copy(s):
        part = lax.rem(s, n_chunk)
        kind = s // n_chunk
        group = jnp.where(kind == 0, 0, 1 + lax.rem(kind - 1 + chip // 2, 2))
        slot = lax.rem(s, DEPTH)
        return pltpu.make_async_copy(w2_buf.at[slot], w2_all.at[group * n_chunk + part], w2_sem.at[slot])

    def w_step(s, first):
        w_start(s + DEPTH - 1)
        w_wait(s)

        @pl.when(s >= 1)
        def _():
            w2_copy(s - 1).start()

        @pl.when(s >= DEPTH)
        def _():
            w2_copy(s - DEPTH).wait()
        part = lax.rem(s, n_chunk)
        w_tile = w_buf[lax.rem(s, DEPTH)].reshape(D_CHUNK, tile_w)
        w2_buf[lax.rem(s, DEPTH)] = w_tile
        add = jnp.dot(xs[:, pl.ds(al(part * D_CHUNK, D_CHUNK), D_CHUNK)], w_tile,
                      preferred_element_type=F32)
        acc[...] = add if first else acc[...] + add

    def w_loop(lo, hi):
        def body(s, carry):
            w_step(s, False)
            return carry
        lax.fori_loop(lo, hi, body, 0)

    def kv_ship(dest_chip, act):
        dest = 2 * dest_chip + core
        lanes = pl.ds(al(dest_chip * head, head), head)
        for k, at in enumerate((low_at, high_at)):
            act(dest == me, st_kv.at[pl.ds(k * rows, rows), lanes], kv_all.at[core, pl.ds(at, rows), :],
                kv_send.at[dest_chip, k], kv_recv.at[chip, k], dest)

    def kv_ship_all(act):
        def body(n, carry):
            kv_ship(lax.rem(n + chip, n_chip), act)
            return carry
        lax.fori_loop(0, n_chip, body, 0)

    def q_ship(t, n, act):
        dest = 4 * tile_of(t) + lax.rem(n + 2 * chip, 4)
        lanes = pl.ds(al(lax.rem(dest, 4) * wide, wide), wide)
        for k, at in enumerate((low_at, high_at)):
            act(dest == me, st_q.at[t, pl.ds(k * rows, rows), lanes], q_all.at[pl.ds(at, rows), :],
                q_send.at[4 * t + n, k], q_recv.at[chip, k], dest)

    def q_ship_all(t, act):
        def body(n, carry):
            q_ship(t, n, act)
            return carry
        lax.fori_loop(0, 4, body, 0)

    w_step(jnp.int32(0), True)
    do_ship(n_dest - 1, ship_start)
    w_loop(1, n_chunk)
    st_kv[...] = acc[...].astype(BF16)
    w_step(jnp.int32(n_chunk), True)
    kv_ship_all(ship_start)
    w_loop(n_chunk + 1, 2 * n_chunk)
    st_q[0] = acc[...].astype(BF16)
    w_step(jnp.int32(2 * n_chunk), True)
    q_ship_all(0, ship_start)
    w_loop(2 * n_chunk + 1, 3 * n_chunk)
    st_q[1] = acc[...].astype(BF16)

    def kv_arrive(src_chip, carry):
        @pl.when(src_chip != chip)
        def _():
            for k in range(2):
                rcopy(st_kv.at[pl.ds(0, rows), pl.ds(0, head)], kv_all.at[core, pl.ds(0, rows), :],
                      kv_send.at[0, k], kv_recv.at[src_chip, k], sib).wait_recv()
        return carry

    lax.fori_loop(0, n_chip, kv_arrive, 0)
    q_ship_all(1, ship_start)
    w2_copy(jnp.int32(3 * n_chunk - 1)).start()
    for k in range(DEPTH):
        w2_copy(jnp.int32(3 * n_chunk - DEPTH + k)).wait()
    kv_ship_all(ship_wait)
    relay = rcopy(kv_all.at[core], kv_all.at[core], rel_send, rel_recv, sib)
    relay.start()

    def wide_arrive(src_chip, carry):
        @pl.when(2 * src_chip + my_src_core != me)
        def _():
            for k in range(2):
                rcopy(st_do.at[0, pl.ds(0, rows), :], do_all.at[pl.ds(0, rows), :],
                      do_send.at[0, k], do_recv.at[src_chip, k], sib).wait_recv()
                rcopy(st_do.at[0, pl.ds(0, rows), :], q_all.at[pl.ds(0, rows), :],
                      q_send.at[0, k], q_recv.at[src_chip, k], sib).wait_recv()
        return carry

    lax.fori_loop(0, n_chip, wide_arrive, 0)

    def do_done(n, carry):
        do_ship(n, ship_wait)
        return carry

    lax.fori_loop(0, n_dest, do_done, 0)
    q_ship_all(0, ship_wait)
    q_ship_all(1, ship_wait)
    rcopy(kv_all.at[core], kv_all.at[1 - core], rel_send, rel_recv, sib).wait_recv()
    relay.wait_send()


def attend_kernel(n_dev, scale, q_ref, do_ref, kv_ref, w2_hbm, dx_ref,
                  k_t, v_t, s_scr, p_scr, dq_st, dkv_acc, dq_in, dkv_in, dkv_far, dkv_st, w2, acc, far,
                  w_sem, dq_send, dq_recv, dkv_send, dkv_recv, far_send, far_recv, red_send, red_recv):
    me, chip, core, sib = place()
    n_chip = n_dev // 2
    rows, d_model = dx_ref.shape
    seg = rows // 2
    seq, wide = q_ref.shape
    head = kv_ref.shape[2]
    heads = wide // head
    n_chunk = d_model // D_CHUNK
    half_dev = n_dev // 2
    dq_core = chip // (n_chip // 2)
    src_slot = lax.rem(me, half_dev)
    n_block = seq // BQ
    to_log2 = scale * 1.4426950408889634

    def w2_copy(group):
        part = pl.ds(group * n_chunk, n_chunk)
        return pltpu.make_async_copy(w2_hbm.at[part], w2.at[part], w_sem.at[group])

    for group in range(3):
        w2_copy(group).start()
    barrier = pltpu.get_barrier_semaphore()

    def greet(step, carry):
        other = lax.rem(me + step, n_dev)
        pl.semaphore_signal(barrier, inc=1, device_id={"cp": other}, device_id_type=MESH)
        return carry

    lax.fori_loop(1, n_dev, greet, 0)
    k_t[...] = kv_ref[0].T
    v_t[...] = kv_ref[1].T
    dkv_acc[...] = jnp.zeros_like(dkv_acc)

    def body(qb):
        q_rows = slice(qb * BQ, (qb + 1) * BQ)
        q = [q_ref[q_rows, h * head:(h + 1) * head] for h in range(heads)]
        do = [do_ref[q_rows, h * head:(h + 1) * head] for h in range(heads)]
        cuts = list(range(0, qb * BQ, BK)) + [qb * BQ, (qb + 1) * BQ]
        chunks = [slice(lo, hi) for lo, hi in zip(cuts[:-1], cuts[1:])]
        tops = [[] for _ in range(heads)]
        sums = [[] for _ in range(heads)]
        for ks in chunks:
            k_blk = kv_ref[0, ks, :]
            for h in range(heads):
                s = lax.dot_general(k_blk, q[h], CONTRACT_LAST, preferred_element_type=F32)
                if ks.start == qb * BQ:
                    k_pos = lax.broadcasted_iota(jnp.int32, (BQ, BQ), 0)
                    q_pos = lax.broadcasted_iota(jnp.int32, (BQ, BQ), 1)
                    s = jnp.where(k_pos <= q_pos, s, -jnp.inf)
                top = jnp.max(s, axis=0, keepdims=True) * to_log2
                e = jnp.exp2(s * to_log2 - top)
                s_scr[h, ks, :] = e
                tops[h].append(top)
                sums[h].append(jnp.sum(e, axis=0, keepdims=True))
        delta = []
        for h in range(heads):
            top = functools.reduce(jnp.maximum, tops[h])
            lift = [jnp.exp2(t - top) for t in tops[h]]
            inv = 1.0 / sum(a * b for a, b in zip(lift, sums[h]))
            o_t = None
            for ks, up in zip(chunks, lift):
                p = (s_scr[h, ks, :] * (up * inv)).astype(BF16)
                p_scr[h, ks, :] = p
                part = jnp.dot(v_t[:, ks], p, preferred_element_type=F32)
                o_t = part if o_t is None else o_t + part
            delta.append(jnp.sum(do[h].astype(F32).T * o_t.astype(BF16).astype(F32), axis=0, keepdims=True))
        dq_t = [None] * heads
        for ks in chunks:
            v_blk = kv_ref[1, ks, :]
            dk = dv = None
            for h in range(heads):
                p = p_scr[h, ks, :]
                dp = lax.dot_general(v_blk, do[h], CONTRACT_LAST, preferred_element_type=F32)
                ds = (p.astype(F32) * (dp - delta[h])).astype(BF16)
                part = jnp.dot(k_t[:, ks], ds, preferred_element_type=F32)
                dq_t[h] = part if dq_t[h] is None else dq_t[h] + part
                dk_h = jnp.dot(ds, q[h], preferred_element_type=F32)
                dv_h = jnp.dot(p, do[h], preferred_element_type=F32)
                dk = dk_h if dk is None else dk + dk_h
                dv = dv_h if dv is None else dv + dv_h
            dkv_acc[0, ks, :] += dk
            dkv_acc[1, ks, :] += dv
        for h in range(heads):
            dq_st[q_rows, h * head:(h + 1) * head] = (dq_t[h] * scale).T.astype(BF16)

    def dq_ship(block, act):
        k = block // n_chip
        dest_chip = jnp.where(k == 0, block, 2 * n_chip - 1 - block)
        dest = 2 * dest_chip + dq_core
        act(dest == me, dq_st.at[pl.ds(al(block * rows, rows), rows), :],
            dq_in.at[src_slot // 4, pl.ds(al(k * rows, rows), rows), pl.ds(al(lax.rem(src_slot, 4) * wide, wide), wide)],
            dq_send.at[block], dq_recv.at[src_slot, k], dest)

    per = BQ // rows

    def turn(step, carry):
        qb = lax.rem(chip + step, n_block)
        for which in range(n_block):
            @pl.when(qb == which)
            def _():
                body(which)

        @pl.when(step == 0)
        def _():
            pl.semaphore_wait(barrier, n_dev - 1)
        for i in range(per):
            dq_ship(qb * per + i, ship_start)
        return carry

    lax.fori_loop(0, n_block, turn, 0)
    swap = rcopy(dkv_acc.at[1 - core], dkv_far, red_send, red_recv, sib)
    swap.start()

    def dkv_ship(n, act):
        dest_chip = lax.rem(chip + n, n_chip)
        dest = 2 * dest_chip + core
        for k in range(2):
            block = dest_chip if k == 0 else 2 * n_chip - 1 - dest_chip
            act(dest == me, dkv_st.at[pl.ds(al(block * rows, rows), rows), :],
                dkv_in.at[pl.ds(k * rows, rows), pl.ds(al(chip * head, head), head)],
                dkv_send.at[n, k], dkv_recv.at[chip, k], dest)

    def each(count, ship, act):
        def step(n, carry):
            ship(n, act)
            return carry
        lax.fori_loop(0, count, step, 0)

    swap.wait()
    factor = jnp.where(core == 0, scale, 1.0).astype(F32)
    dkv_st[...] = ((dkv_acc[core] + dkv_far[...]) * factor).astype(BF16)
    for group in range(3):
        w2_copy(group).wait()
    each(n_chip, dkv_ship, ship_start)

    def dq_arrive(src, carry):
        @pl.when(half_dev * core + src != me)
        def _():
            for k in range(2):
                rcopy(dq_st.at[pl.ds(0, rows), :], dq_in.at[0, pl.ds(0, rows), pl.ds(0, wide)],
                      dq_send.at[0], dq_recv.at[src, k], sib).wait_recv()
        return carry

    def matmul(act, base, part):
        return lax.dot_general(act, w2[base + part], CONTRACT_LAST, preferred_element_type=F32)

    each(n_block * per, dq_ship, ship_wait)
    lax.fori_loop(0, half_dev, dq_arrive, 0)

    def first_pass(part, carry):
        acc[part] = matmul(dq_in[0], n_chunk, part) + matmul(dq_in[1], 2 * n_chunk, part)
        return carry

    lax.fori_loop(0, n_chunk, first_pass, 0)
    each(n_chip, dkv_ship, ship_wait)

    def dkv_arrive(src_chip, carry):
        @pl.when(src_chip != chip)
        def _():
            for k in range(2):
                rcopy(dkv_st.at[pl.ds(0, rows), :], dkv_in.at[pl.ds(0, rows), pl.ds(0, head)],
                      dkv_send.at[0, k], dkv_recv.at[src_chip, k], sib).wait_recv()
        return carry

    lax.fori_loop(0, n_chip, dkv_arrive, 0)

    sib_low = al((1 - core) * seg, seg)
    sib_high = al(rows + core * seg, seg)
    my_low = al(core * seg, seg)
    my_high = al(rows + (1 - core) * seg, seg)

    def far_copy(part, k):
        src_at = sib_low if k == 0 else sib_high
        return rcopy(acc.at[part, pl.ds(src_at, seg), :], far.at[part, pl.ds(k * seg, seg), :],
                     far_send.at[part, k], far_recv.at[part, k], sib)

    def last_pass(part, carry):
        acc[part] += matmul(dkv_in[...], 0, part)

        @pl.when(part > 0)
        def _():
            for k in range(2):
                far_copy(part - 1, k).start()
        return carry

    lax.fori_loop(0, n_chunk, last_pass, 0)
    for k in range(2):
        far_copy(n_chunk - 1, k).start()

    def finish(part, carry):
        for k in range(2):
            far_copy(part, k).wait()
        lanes = pl.ds(al(part * D_CHUNK, D_CHUNK), D_CHUNK)
        dx_ref[pl.ds(0, seg), lanes] = (acc[part, pl.ds(my_low, seg), :] + far[part, pl.ds(0, seg), :]).astype(BF16)
        dx_ref[pl.ds(seg, seg), lanes] = (acc[part, pl.ds(my_high, seg), :] + far[part, pl.ds(seg, seg), :]).astype(BF16)
        return carry

    lax.fori_loop(0, n_chunk, finish, 0)


def solution(mesh):
    n_dev = mesh.shape["cp"]
    n_chip = n_dev // 2
    row_spec = P(("dp", "cp"), None)
    any_spec = pl.BlockSpec(memory_space=pl.ANY)
    vmem_spec = pl.BlockSpec(memory_space=pltpu.VMEM)
    dma = pltpu.SemaphoreType.DMA

    def device_fn(x_in, d_y, w_q, w_k, w_v, w_o):
        rows, d_model = x_in.shape
        q_heads, head = w_q.shape[1], w_q.shape[2]
        kv_heads = w_k.shape[1]
        seq = rows * n_dev
        scale = head ** -0.5
        wide = q_heads // n_dev * head
        tile_w = kv_heads * head
        n_chunk = d_model // D_CHUNK
        wo_flat = w_o.reshape(q_heads * head, d_model)
        params = functools.partial(pltpu.CompilerParams, vmem_limit_bytes=VMEM_LIMIT)
        q_all, do_all, kv_all, w2_all = pl.pallas_call(
            functools.partial(project_kernel, n_dev),
            out_shape=(jax.ShapeDtypeStruct((seq, wide), BF16),
                       jax.ShapeDtypeStruct((seq, wide), BF16),
                       jax.ShapeDtypeStruct((2, seq, head), BF16),
                       jax.ShapeDtypeStruct((3 * n_chunk, D_CHUNK, tile_w), BF16)),
            in_specs=[vmem_spec, vmem_spec, any_spec, any_spec, any_spec, any_spec],
            out_specs=[any_spec] * 4,
            scratch_shapes=[
                pltpu.VMEM((2 * rows, d_model), BF16),
                pltpu.VMEM((2 * rows, d_model), BF16),
                pltpu.VMEM((WO_DEPTH, wide, d_model), BF16),
                pltpu.VMEM((DEPTH, D_CHUNK, kv_heads, head), BF16),
                pltpu.VMEM((DEPTH, D_CHUNK, tile_w), BF16),
                pltpu.VMEM((2 * rows, tile_w), F32),
                pltpu.VMEM((n_chip, 2 * rows, wide), BF16),
                pltpu.VMEM((2 * rows, tile_w), BF16),
                pltpu.VMEM((2, 2 * rows, tile_w), BF16),
                dma((WO_DEPTH,)), dma((DEPTH,)), dma((DEPTH,)), dma((2, 2)), dma((2, 2)),
                dma((n_chip, 2)), dma((n_chip, 2)), dma((n_chip, 2)), dma((n_chip, 2)),
                dma((n_chip, 2)), dma((n_chip, 2)), dma, dma,
            ],
            compiler_params=params(collective_id=0, has_side_effects=True),
            name="project",
        )(x_in, d_y, w_q, w_k, w_v, wo_flat)
        return pl.pallas_call(
            functools.partial(attend_kernel, n_dev, scale),
            out_shape=jax.ShapeDtypeStruct((rows, d_model), BF16),
            in_specs=[vmem_spec, vmem_spec, vmem_spec, any_spec],
            out_specs=vmem_spec,
            scratch_shapes=[
                pltpu.VMEM((head, seq), BF16),
                pltpu.VMEM((head, seq), BF16),
                pltpu.VMEM((wide // head, seq, BQ), F32),
                pltpu.VMEM((wide // head, seq, BQ), BF16),
                pltpu.VMEM((seq, wide), BF16),
                pltpu.VMEM((2, seq, head), F32),
                pltpu.VMEM((2, 2 * rows, tile_w), BF16),
                pltpu.VMEM((2 * rows, tile_w), BF16),
                pltpu.VMEM((seq, head), F32),
                pltpu.VMEM((seq, head), BF16),
                pltpu.VMEM((3 * n_chunk, D_CHUNK, tile_w), BF16),
                pltpu.VMEM((n_chunk, 2 * rows, D_CHUNK), F32),
                pltpu.VMEM((n_chunk, rows, D_CHUNK), F32),
                dma((3,)), dma((seq // rows,)), dma((n_chip, 2)), dma((n_chip, 2)), dma((n_chip, 2)),
                dma((n_chunk, 2)), dma((n_chunk, 2)), dma, dma,
            ],
            compiler_params=params(collective_id=1, has_side_effects=True),
            name="attend",
        )(q_all, do_all, kv_all, w2_all)

    return jax.shard_map(device_fn, mesh=mesh, in_specs=(row_spec, row_spec, P(), P(), P(), P()),
                         out_specs=row_spec, check_vma=False)
```

```python
import functools

import jax
import jax.numpy as jnp
from jax import lax
from jax.experimental import pallas as pl
from jax.experimental.pallas import tpu as pltpu
from jax.sharding import PartitionSpec as P

MESH = pl.DeviceIdType.MESH
BF16 = jnp.bfloat16
F32 = jnp.float32
CONTRACT_LAST = (((1,), (1,)), ((), ()))
DEPTH = 4
WO_DEPTH = 2
D_CHUNK = 512
BQ = 256
BK = 512
DO_FIRST = 2
VMEM_LIMIT = 62 * 2 ** 20


def place():
    me = lax.axis_index("cp")
    chip = me // 2
    core = me % 2
    return me, chip, core, me + 1 - 2 * core


def meet_group(n_dev):
    me = lax.axis_index("cp")
    barrier = pltpu.get_barrier_semaphore()

    def greet(step, carry):
        other = lax.rem(me + step, n_dev)
        pl.semaphore_signal(barrier, inc=1, device_id={"cp": other}, device_id_type=MESH)
        return carry

    lax.fori_loop(1, n_dev, greet, 0)
    pl.semaphore_wait(barrier, n_dev - 1)


def rcopy(src, dst, send_sem, recv_sem, dev):
    return pltpu.make_async_remote_copy(
        src_ref=src, dst_ref=dst, send_sem=send_sem, recv_sem=recv_sem,
        device_id={"cp": dev}, device_id_type=MESH)


def al(value, step):
    return pl.multiple_of(value, step)


def ship_start(is_me, src, dst, send_sem, recv_sem, dev):
    @pl.when(is_me)
    def _():
        pltpu.make_async_copy(src, dst, send_sem).start()

    @pl.when(jnp.logical_not(is_me))
    def _():
        rcopy(src, dst, send_sem, recv_sem, dev).start()


def ship_wait(is_me, src, dst, send_sem, recv_sem, dev):
    @pl.when(is_me)
    def _():
        pltpu.make_async_copy(src, dst, send_sem).wait()

    @pl.when(jnp.logical_not(is_me))
    def _():
        rcopy(src, dst, send_sem, recv_sem, dev).wait_send()


def fused_kernel(n_dev, scale, x_ref, dy_ref, wq, wk, wv, wo, dx_ref, w2_all,
                 xs, dys, wo_buf, w_buf, w2_buf, p_acc, st_do, st_kv, st_q,
                 q_all, do_all, kv_all, k_t, v_t, p_all, o_all, dq_st, dkv_acc,
                 dq_in, dkv_in, dkv_far, dkv_st, acc, far,
                 wo_sem, w_sem, w2_sem, x_send, x_recv, do_send, do_recv,
                 kv_send, kv_recv, q_send, q_recv, rel_send, rel_recv,
                 dq_send, dq_recv, dkv_send, dkv_recv, far_send, far_recv, red_send, red_recv):
    me, chip, core, sib = place()
    n_chip = n_dev // 2
    rows, d_model = x_ref.shape
    seg = rows // 2
    seq, wide = q_all.shape
    head = kv_all.shape[2]
    heads = wide // head
    tile_w = p_acc.shape[1]
    n_chunk = d_model // D_CHUNK
    n_dest = n_dev // 2
    tile_heads = w_buf.shape[2]
    my_src_core = chip // (n_chip // 2)
    low_at = al(chip * rows, rows)
    high_at = al((2 * n_chip - 1 - chip) * rows, rows)
    n_block = seq // BQ
    per = BQ // rows
    to_log2 = scale * 1.4426950408889634

    def dest_of(n):
        return n_dest * core + lax.rem(2 * n_chip + 2 * chip - 2 * (n // 2) + lax.rem(n, 2), n_dest)

    def wo_copy(n):
        return pltpu.make_async_copy(
            wo.at[pl.ds(al(dest_of(n) * wide, wide), wide), :], wo_buf.at[lax.rem(n, WO_DEPTH)],
            wo_sem.at[lax.rem(n, WO_DEPTH)])

    def tile_of(t):
        return 2 * core + lax.rem(t + chip // 2, 2)

    def w_start(s):
        slot = lax.rem(s, DEPTH)
        part = lax.rem(s, n_chunk)
        d_rows = pl.ds(al(part * D_CHUNK, D_CHUNK), D_CHUNK)

        @pl.when((s < n_chunk) & (core == 0))
        def _():
            pltpu.make_async_copy(wk.at[d_rows], w_buf.at[slot], w_sem.at[slot]).start()

        @pl.when((s < n_chunk) & (core == 1))
        def _():
            pltpu.make_async_copy(wv.at[d_rows], w_buf.at[slot], w_sem.at[slot]).start()

        @pl.when((s >= n_chunk) & (s < 3 * n_chunk))
        def _():
            tile = tile_of(s // n_chunk - 1)
            pltpu.make_async_copy(
                wq.at[d_rows, pl.ds(al(tile * tile_heads, tile_heads), tile_heads), :],
                w_buf.at[slot], w_sem.at[slot]).start()

    def w_wait(s):
        slot = lax.rem(s, DEPTH)
        pltpu.make_async_copy(wk.at[pl.ds(0, D_CHUNK)], w_buf.at[slot], w_sem.at[slot]).wait()

    for n in range(WO_DEPTH - 1):
        wo_copy(jnp.int32(n)).start()
    for s in range(DEPTH - 1):
        w_start(jnp.int32(s))

    my_low = al(core * seg, seg)
    my_high = al(rows + (1 - core) * seg, seg)
    for ref, stack in ((dy_ref, dys), (x_ref, xs)):
        stack[pl.ds(my_low, seg), :] = ref[:seg, :]
        stack[pl.ds(my_high, seg), :] = ref[seg:, :]
    dkv_acc[...] = jnp.zeros_like(dkv_acc)
    meet_group(n_dev)
    swaps = []
    for k, (ref, stack) in enumerate(((dy_ref, dys), (x_ref, xs))):
        swaps.append(rcopy(ref.at[pl.ds(0, seg)], stack.at[pl.ds(my_low, seg)],
                           x_send.at[k, 0], x_recv.at[k, 0], sib))
        swaps.append(rcopy(ref.at[pl.ds(seg, seg)], stack.at[pl.ds(my_high, seg)],
                           x_send.at[k, 1], x_recv.at[k, 1], sib))
    for swap in swaps:
        swap.start()
    swaps[0].wait()
    swaps[1].wait()

    def each(lo, hi, ship, act):
        def step(n, carry):
            ship(n, act)
            return carry
        lax.fori_loop(lo, hi, step, 0)

    def do_ship(n, act):
        dest = dest_of(n)
        for k, at in enumerate((low_at, high_at)):
            act(dest == me, st_do.at[n, pl.ds(k * rows, rows), :], do_all.at[pl.ds(at, rows), :],
                do_send.at[n, k], do_recv.at[chip, k], dest)

    def do_loop(lo, hi):
        def do_step(n, carry):
            @pl.when(n + WO_DEPTH - 1 < n_dest)
            def _():
                wo_copy(n + WO_DEPTH - 1).start()
            wo_copy(n).wait()

            @pl.when(n > lo)
            def _():
                do_ship(n - 1, ship_start)
            st_do[n] = lax.dot_general(dys[...], wo_buf[lax.rem(n, WO_DEPTH)], CONTRACT_LAST,
                                       preferred_element_type=F32).astype(BF16)
            return carry
        lax.fori_loop(lo, hi, do_step, 0)

    do_loop(0, DO_FIRST)
    swaps[2].wait()
    swaps[3].wait()

    def w2_copy(s):
        part = lax.rem(s, n_chunk)
        kind = s // n_chunk
        group = jnp.where(kind == 0, 0, 1 + lax.rem(kind - 1 + chip // 2, 2))
        slot = lax.rem(s, DEPTH)
        return pltpu.make_async_copy(w2_buf.at[slot], w2_all.at[group * n_chunk + part], w2_sem.at[slot])

    def w_step(s, first):
        w_start(s + DEPTH - 1)
        w_wait(s)

        @pl.when(s >= 1)
        def _():
            w2_copy(s - 1).start()

        @pl.when(s >= DEPTH)
        def _():
            w2_copy(s - DEPTH).wait()
        part = lax.rem(s, n_chunk)
        w_tile = w_buf[lax.rem(s, DEPTH)].reshape(D_CHUNK, tile_w)
        w2_buf[lax.rem(s, DEPTH)] = w_tile
        add = jnp.dot(xs[:, pl.ds(al(part * D_CHUNK, D_CHUNK), D_CHUNK)], w_tile,
                      preferred_element_type=F32)
        p_acc[...] = add if first else p_acc[...] + add

    def w_loop(lo, hi):
        def body(s, carry):
            w_step(s, False)
            return carry
        lax.fori_loop(lo, hi, body, 0)

    def kv_ship(n, act):
        dest_chip = lax.rem(n + chip, n_chip)
        dest = 2 * dest_chip + core
        lanes = pl.ds(al(dest_chip * head, head), head)
        for k, at in enumerate((low_at, high_at)):
            act(dest == me, st_kv.at[pl.ds(k * rows, rows), lanes], kv_all.at[core, pl.ds(at, rows), :],
                kv_send.at[dest_chip, k], kv_recv.at[chip, k], dest)

    def q_ship(n, act):
        t = n // 4
        dest = 4 * tile_of(t) + lax.rem(n + 2 * chip, 4)
        lanes = pl.ds(al(lax.rem(dest, 4) * wide, wide), wide)
        for k, at in enumerate((low_at, high_at)):
            act(dest == me, st_q.at[t, pl.ds(k * rows, rows), lanes], q_all.at[pl.ds(at, rows), :],
                q_send.at[n, k], q_recv.at[chip, k], dest)

    w_step(jnp.int32(0), True)
    do_ship(jnp.int32(DO_FIRST - 1), ship_start)
    w_loop(1, n_chunk)
    st_kv[...] = p_acc[...].astype(BF16)
    w_step(jnp.int32(n_chunk), True)
    each(0, n_chip, kv_ship, ship_start)
    w_loop(n_chunk + 1, 2 * n_chunk)
    st_q[0] = p_acc[...].astype(BF16)
    w_step(jnp.int32(2 * n_chunk), True)
    each(0, 4, q_ship, ship_start)
    w_loop(2 * n_chunk + 1, 3 * n_chunk)
    st_q[1] = p_acc[...].astype(BF16)
    w2_copy(jnp.int32(3 * n_chunk - 1)).start()

    def kv_arrive(src_chip, carry):
        @pl.when(src_chip != chip)
        def _():
            for k in range(2):
                rcopy(st_kv.at[pl.ds(0, rows), pl.ds(0, head)], kv_all.at[core, pl.ds(0, rows), :],
                      kv_send.at[0, k], kv_recv.at[src_chip, k], sib).wait_recv()
        return carry

    do_loop(DO_FIRST, DO_FIRST + 1)
    each(4, 8, q_ship, ship_start)
    do_ship(jnp.int32(DO_FIRST), ship_start)
    do_loop(DO_FIRST + 1, n_dest)
    for k in range(DEPTH):
        w2_copy(jnp.int32(3 * n_chunk - DEPTH + k)).wait()
    lax.fori_loop(0, n_chip, kv_arrive, 0)
    do_ship(jnp.int32(n_dest - 1), ship_start)
    each(0, n_chip, kv_ship, ship_wait)
    relay = rcopy(kv_all.at[core], kv_all.at[core], rel_send, rel_recv, sib)
    relay.start()

    def q_arrive(src_chip, carry):
        @pl.when(2 * src_chip + my_src_core != me)
        def _():
            for k in range(2):
                rcopy(st_do.at[0, pl.ds(0, rows), :], q_all.at[pl.ds(0, rows), :],
                      q_send.at[0, k], q_recv.at[src_chip, k], sib).wait_recv()
        return carry

    rcopy(kv_all.at[core], kv_all.at[1 - core], rel_send, rel_recv, sib).wait_recv()
    relay.wait_send()
    k_t[...] = kv_all[0].T
    v_t[...] = kv_all[1].T
    each(0, 8, q_ship, ship_wait)
    lax.fori_loop(0, n_chip, q_arrive, 0)

    def chunks_of(qb):
        cuts = list(range(0, qb * BQ, BK)) + [qb * BQ, (qb + 1) * BQ]
        return [slice(lo, hi) for lo, hi in zip(cuts[:-1], cuts[1:])]

    def s_at(ks):
        return slice(ks.start // BQ, ks.stop // BQ)

    def p_rows(qb, ks):
        base = BQ * (qb * (qb + 1) // 2)
        return slice(base + ks.start, base + ks.stop)

    def forward(qb):
        q_rows = slice(qb * BQ, (qb + 1) * BQ)
        q = [q_all[q_rows, h * head:(h + 1) * head] for h in range(heads)]
        chunks = chunks_of(qb)
        tops = [[] for _ in range(heads)]
        sums = [[] for _ in range(heads)]
        for ks in chunks:
            k_blk = kv_all[0, ks, :]
            for h in range(heads):
                s = lax.dot_general(k_blk, q[h], CONTRACT_LAST, preferred_element_type=F32)
                if ks.start == qb * BQ:
                    k_pos = lax.broadcasted_iota(jnp.int32, (BQ, BQ), 0)
                    q_pos = lax.broadcasted_iota(jnp.int32, (BQ, BQ), 1)
                    s = jnp.where(k_pos <= q_pos, s, -jnp.inf)
                top = jnp.max(s, axis=0, keepdims=True) * to_log2
                e = jnp.exp2(s * to_log2 - top)
                acc[s_at(ks), :, h * BQ:(h + 1) * BQ] = e.reshape(-1, BQ, BQ)
                tops[h].append(top)
                sums[h].append(jnp.sum(e, axis=0, keepdims=True))
        for h in range(heads):
            top = functools.reduce(jnp.maximum, tops[h])
            lift = [jnp.exp2(t - top) for t in tops[h]]
            inv = 1.0 / sum(a * b for a, b in zip(lift, sums[h]))
            o_t = None
            for ks, up in zip(chunks, lift):
                p = (acc[s_at(ks), :, h * BQ:(h + 1) * BQ].reshape(-1, BQ) * (up * inv)).astype(BF16)
                p_all[h, p_rows(qb, ks), :] = p
                part = jnp.dot(v_t[:, ks], p, preferred_element_type=F32)
                o_t = part if o_t is None else o_t + part
            o_all[h, :, q_rows] = o_t.astype(BF16)

    def backward(qb):
        q_rows = slice(qb * BQ, (qb + 1) * BQ)
        q = [q_all[q_rows, h * head:(h + 1) * head] for h in range(heads)]
        do = [do_all[q_rows, h * head:(h + 1) * head] for h in range(heads)]
        delta = [jnp.sum(do[h].astype(F32).T * o_all[h, :, q_rows].astype(F32), axis=0, keepdims=True)
                 for h in range(heads)]
        dq_t = [None] * heads
        for ks in chunks_of(qb):
            v_blk = kv_all[1, ks, :]
            dk = dv = None
            for h in range(heads):
                p = p_all[h, p_rows(qb, ks), :]
                dp = lax.dot_general(v_blk, do[h], CONTRACT_LAST, preferred_element_type=F32)
                ds = (p.astype(F32) * (dp - delta[h])).astype(BF16)
                part = jnp.dot(k_t[:, ks], ds, preferred_element_type=F32)
                dq_t[h] = part if dq_t[h] is None else dq_t[h] + part
                dk_h = jnp.dot(ds, q[h], preferred_element_type=F32)
                dv_h = jnp.dot(p, do[h], preferred_element_type=F32)
                dk = dk_h if dk is None else dk + dk_h
                dv = dv_h if dv is None else dv + dv_h
            dkv_acc[0, ks, :] += dk
            dkv_acc[1, ks, :] += dv
        for h in range(heads):
            dq_st[q_rows, h * head:(h + 1) * head] = (dq_t[h] * scale).T.astype(BF16)

    def block_at(step):
        side = lax.rem(lax.rem(chip, 4) // 2 + step // 4, 2)
        spot = lax.rem(step + lax.rem(chip, 2) + 2 * (chip // 4), 4)
        return jnp.where(spot < 2, 2 * spot + side, 11 - 2 * spot - side)

    def home_of(block):
        return jnp.where(block < n_chip, block, 2 * n_chip - 1 - block)

    def ahead(step, carry):
        qb = block_at(step)
        for which in range(n_block):
            @pl.when(qb == which)
            def _():
                forward(which)
        return carry

    lax.fori_loop(0, n_block, ahead, 0)

    src_slot = lax.rem(me, n_dest)

    def dq_ship(block, act):
        k = block // n_chip
        dest = 2 * home_of(block) + my_src_core
        act(dest == me, dq_st.at[pl.ds(al(block * rows, rows), rows), :],
            dq_in.at[src_slot // 4, pl.ds(al(k * rows, rows), rows), pl.ds(al(lax.rem(src_slot, 4) * wide, wide), wide)],
            dq_send.at[block], dq_recv.at[src_slot, k], dest)

    def do_done(n, carry):
        @pl.when(dest_of(n) == me)
        def _():
            do_ship(n, ship_wait)
        return carry

    lax.fori_loop(0, n_dest, do_done, 0)

    def back(step, carry):
        qb = block_at(step)
        for i in range(per):
            block = qb * per + i
            home = home_of(block)

            @pl.when(2 * home + my_src_core != me)
            def _():
                rcopy(st_do.at[0, pl.ds(0, rows), :], do_all.at[pl.ds(0, rows), :],
                      do_send.at[0, 0], do_recv.at[home, block // n_chip], sib).wait_recv()
        for which in range(n_block):
            @pl.when(qb == which)
            def _():
                backward(which)
        for i in range(per):
            dq_ship(qb * per + i, ship_start)
        return carry

    lax.fori_loop(0, n_block, back, 0)
    swap = rcopy(dkv_acc.at[1 - core], dkv_far, red_send, red_recv, sib)
    swap.start()

    def stream_copy(u):
        group = jnp.where(u < 2 * n_chunk, 1 + lax.rem(u, 2), 0)
        part = jnp.where(u < 2 * n_chunk, u // 2, u - 2 * n_chunk)
        slot = lax.rem(u, DEPTH)
        return pltpu.make_async_copy(w2_all.at[group * n_chunk + part], w2_buf.at[slot], w2_sem.at[slot])

    for u in range(DEPTH - 1):
        stream_copy(jnp.int32(u)).start()

    def do_sent(n, carry):
        @pl.when(dest_of(n) != me)
        def _():
            do_ship(n, ship_wait)
        return carry

    lax.fori_loop(0, n_dest, do_sent, 0)

    def dkv_ship(n, act):
        dest_chip = lax.rem(chip + n, n_chip)
        dest = 2 * dest_chip + core
        for k in range(2):
            block = dest_chip if k == 0 else 2 * n_chip - 1 - dest_chip
            act(dest == me, dkv_st.at[pl.ds(al(block * rows, rows), rows), :],
                dkv_in.at[pl.ds(k * rows, rows), pl.ds(al(chip * head, head), head)],
                dkv_send.at[n, k], dkv_recv.at[chip, k], dest)

    swap.wait()
    factor = jnp.where(core == 0, scale, 1.0).astype(F32)
    dkv_st[...] = ((dkv_acc[core] + dkv_far[...]) * factor).astype(BF16)
    each(0, n_block * per, dq_ship, ship_wait)
    each(0, n_chip, dkv_ship, ship_start)

    def dq_arrive(src, carry):
        @pl.when(n_dest * core + src != me)
        def _():
            for k in range(2):
                rcopy(dq_st.at[pl.ds(0, rows), :], dq_in.at[0, pl.ds(0, rows), pl.ds(0, wide)],
                      dq_send.at[0], dq_recv.at[src, k], sib).wait_recv()
        return carry

    lax.fori_loop(0, n_dest, dq_arrive, 0)

    def matmul(act, u):
        @pl.when(u + DEPTH - 1 < 3 * n_chunk)
        def _():
            stream_copy(u + DEPTH - 1).start()
        stream_copy(u).wait()
        return lax.dot_general(act, w2_buf[lax.rem(u, DEPTH)], CONTRACT_LAST, preferred_element_type=F32)

    def first_pass(part, carry):
        acc[part] = matmul(dq_in[0], 2 * part)
        acc[part] += matmul(dq_in[1], 2 * part + 1)
        return carry

    lax.fori_loop(0, n_chunk, first_pass, 0)
    each(0, n_chip, dkv_ship, ship_wait)

    def dkv_arrive(src_chip, carry):
        @pl.when(src_chip != chip)
        def _():
            for k in range(2):
                rcopy(dkv_st.at[pl.ds(0, rows), :], dkv_in.at[pl.ds(0, rows), pl.ds(0, head)],
                      dkv_send.at[0, k], dkv_recv.at[src_chip, k], sib).wait_recv()
        return carry

    lax.fori_loop(0, n_chip, dkv_arrive, 0)

    sib_low = al((1 - core) * seg, seg)
    sib_high = al(rows + core * seg, seg)

    def far_copy(part, k):
        src_at = sib_low if k == 0 else sib_high
        return rcopy(acc.at[part, pl.ds(src_at, seg), :], far.at[part, pl.ds(k * seg, seg), :],
                     far_send.at[part, k], far_recv.at[part, k], sib)

    def last_pass(part, carry):
        acc[part] += matmul(dkv_in[...], 2 * n_chunk + part)

        @pl.when(part > 0)
        def _():
            for k in range(2):
                far_copy(part - 1, k).start()
        return carry

    lax.fori_loop(0, n_chunk, last_pass, 0)
    for k in range(2):
        far_copy(n_chunk - 1, k).start()

    def finish(part, carry):
        for k in range(2):
            far_copy(part, k).wait()
        lanes = pl.ds(al(part * D_CHUNK, D_CHUNK), D_CHUNK)
        dx_ref[pl.ds(0, seg), lanes] = (acc[part, pl.ds(my_low, seg), :] + far[part, pl.ds(0, seg), :]).astype(BF16)
        dx_ref[pl.ds(seg, seg), lanes] = (acc[part, pl.ds(my_high, seg), :] + far[part, pl.ds(seg, seg), :]).astype(BF16)
        return carry

    lax.fori_loop(0, n_chunk, finish, 0)


def solution(mesh):
    n_dev = mesh.shape["cp"]
    n_chip = n_dev // 2
    row_spec = P(("dp", "cp"), None)
    any_spec = pl.BlockSpec(memory_space=pl.ANY)
    vmem_spec = pl.BlockSpec(memory_space=pltpu.VMEM)
    dma = pltpu.SemaphoreType.DMA

    def device_fn(x_in, d_y, w_q, w_k, w_v, w_o):
        rows, d_model = x_in.shape
        q_heads, head = w_q.shape[1], w_q.shape[2]
        kv_heads = w_k.shape[1]
        seq = rows * n_dev
        scale = head ** -0.5
        wide = q_heads // n_dev * head
        tile_w = kv_heads * head
        n_chunk = d_model // D_CHUNK
        wo_flat = w_o.reshape(q_heads * head, d_model)
        params = functools.partial(pltpu.CompilerParams, vmem_limit_bytes=VMEM_LIMIT)
        tri = (seq // BQ) * (seq // BQ + 1) // 2 * BQ
        return pl.pallas_call(
            functools.partial(fused_kernel, n_dev, scale),
            out_shape=(jax.ShapeDtypeStruct((rows, d_model), BF16),
                       jax.ShapeDtypeStruct((3 * n_chunk, D_CHUNK, tile_w), BF16)),
            in_specs=[vmem_spec, vmem_spec, any_spec, any_spec, any_spec, any_spec],
            out_specs=(vmem_spec, any_spec),
            scratch_shapes=[
                pltpu.VMEM((2 * rows, d_model), BF16),
                pltpu.VMEM((2 * rows, d_model), BF16),
                pltpu.VMEM((WO_DEPTH, wide, d_model), BF16),
                pltpu.VMEM((DEPTH, D_CHUNK, kv_heads, head), BF16),
                pltpu.VMEM((DEPTH, D_CHUNK, tile_w), BF16),
                pltpu.VMEM((2 * rows, tile_w), F32),
                pltpu.VMEM((n_chip, 2 * rows, wide), BF16),
                pltpu.VMEM((2 * rows, tile_w), BF16),
                pltpu.VMEM((2, 2 * rows, tile_w), BF16),
                pltpu.VMEM((seq, wide), BF16),
                pltpu.VMEM((seq, wide), BF16),
                pltpu.VMEM((2, seq, head), BF16),
                pltpu.VMEM((head, seq), BF16),
                pltpu.VMEM((head, seq), BF16),
                pltpu.VMEM((wide // head, tri, BQ), BF16),
                pltpu.VMEM((wide // head, head, seq), BF16),
                pltpu.VMEM((seq, wide), BF16),
                pltpu.VMEM((2, seq, head), F32),
                pltpu.VMEM((2, 2 * rows, tile_w), BF16),
                pltpu.VMEM((2 * rows, tile_w), BF16),
                pltpu.VMEM((seq, head), F32),
                pltpu.VMEM((seq, head), BF16),
                pltpu.VMEM((n_chunk, 2 * rows, D_CHUNK), F32),
                pltpu.VMEM((n_chunk, rows, D_CHUNK), F32),
                dma((WO_DEPTH,)), dma((DEPTH,)), dma((DEPTH,)), dma((2, 2)), dma((2, 2)),
                dma((n_chip, 2)), dma((n_chip, 2)), dma((n_chip, 2)), dma((n_chip, 2)),
                dma((n_chip, 2)), dma((n_chip, 2)), dma, dma,
                dma((seq // rows,)), dma((n_chip, 2)), dma((n_chip, 2)), dma((n_chip, 2)),
                dma((n_chunk, 2)), dma((n_chunk, 2)), dma, dma,
            ],
            compiler_params=params(collective_id=0, has_side_effects=True),
            name="fused",
        )(x_in, d_y, w_q, w_k, w_v, wo_flat)[0]

    return jax.shard_map(device_fn, mesh=mesh, in_specs=(row_spec, row_spec, P(), P(), P(), P()),
                         out_specs=row_spec, check_vma=False)
```

```python
import functools

import jax
import jax.numpy as jnp
from jax import lax
from jax.experimental import pallas as pl
from jax.experimental.pallas import tpu as pltpu
from jax.sharding import PartitionSpec as P

MESH = pl.DeviceIdType.MESH
BF16 = jnp.bfloat16
F32 = jnp.float32
CONTRACT_LAST = (((1,), (1,)), ((), ()))
DEPTH = 4
W2_DEPTH = 6
WO_DEPTH = 2
D_CHUNK = 512
BQ = 256
BK = 512
DO_FIRST = 2
VMEM_LIMIT = 62 * 2 ** 20


def place():
    me = lax.axis_index("cp")
    chip = me // 2
    core = me % 2
    return me, chip, core, me + 1 - 2 * core


def meet_group(n_dev):
    me = lax.axis_index("cp")
    barrier = pltpu.get_barrier_semaphore()

    def greet(step, carry):
        other = lax.rem(me + step, n_dev)
        pl.semaphore_signal(barrier, inc=1, device_id={"cp": other}, device_id_type=MESH)
        return carry

    lax.fori_loop(1, n_dev, greet, 0)
    pl.semaphore_wait(barrier, n_dev - 1)


def rcopy(src, dst, send_sem, recv_sem, dev):
    return pltpu.make_async_remote_copy(
        src_ref=src, dst_ref=dst, send_sem=send_sem, recv_sem=recv_sem,
        device_id={"cp": dev}, device_id_type=MESH)


def al(value, step):
    return pl.multiple_of(value, step)


def ship_start(is_me, src, dst, send_sem, recv_sem, dev):
    @pl.when(is_me)
    def _():
        pltpu.make_async_copy(src, dst, send_sem).start()

    @pl.when(jnp.logical_not(is_me))
    def _():
        rcopy(src, dst, send_sem, recv_sem, dev).start()


def ship_wait(is_me, src, dst, send_sem, recv_sem, dev):
    @pl.when(is_me)
    def _():
        pltpu.make_async_copy(src, dst, send_sem).wait()

    @pl.when(jnp.logical_not(is_me))
    def _():
        rcopy(src, dst, send_sem, recv_sem, dev).wait_send()


def fused_kernel(n_dev, scale, x_ref, dy_ref, wq, wk, wv, wo, dx_ref, w2_all,
                 xs, dys, wo_buf, w_buf, w2_buf, p_acc, st_do, st_kv, st_q,
                 q_all, do_all, kv_all, k_t, v_t, p_all, o_all, dq_st, dkv_acc,
                 dq_in, dkv_in, dkv_far, dkv_st, grads_t, acc, far,
                 wo_sem, w_sem, w2_sem, x_send, x_recv, do_send, do_recv,
                 kv_send, kv_recv, q_send, q_recv, rel_send, rel_recv,
                 dq_send, dq_recv, dkv_send, dkv_recv, far_send, far_recv, red_send, red_recv):
    me, chip, core, sib = place()
    n_chip = n_dev // 2
    rows, d_model = x_ref.shape
    seg = rows // 2
    seq, wide = q_all.shape
    head = kv_all.shape[2]
    heads = wide // head
    tile_w = p_acc.shape[1]
    n_chunk = d_model // D_CHUNK
    n_dest = n_dev // 2
    tile_heads = w_buf.shape[2]
    my_src_core = chip // (n_chip // 2)
    low_at = al(chip * rows, rows)
    high_at = al((2 * n_chip - 1 - chip) * rows, rows)
    n_block = seq // BQ
    per = BQ // rows
    to_log2 = scale * 1.4426950408889634

    def dest_of(n):
        spot, step = lax.rem(chip, 4), n // 2
        flip = 2 * lax.rem(spot // 2 + step // 2, 2) + lax.rem(spot + step, 2)
        return n_dest * core + 2 * flip + lax.rem(n, 2)

    def wo_copy(n):
        return pltpu.make_async_copy(
            wo.at[pl.ds(al(dest_of(n) * wide, wide), wide), :], wo_buf.at[lax.rem(n, WO_DEPTH)],
            wo_sem.at[lax.rem(n, WO_DEPTH)])

    def tile_of(t):
        return 2 * core + lax.rem(t + chip // 2, 2)

    def w_start(s):
        slot = lax.rem(s, DEPTH)
        part = lax.rem(s, n_chunk)
        d_rows = pl.ds(al(part * D_CHUNK, D_CHUNK), D_CHUNK)

        @pl.when((s < n_chunk) & (core == 0))
        def _():
            pltpu.make_async_copy(wk.at[d_rows], w_buf.at[slot], w_sem.at[slot]).start()

        @pl.when((s < n_chunk) & (core == 1))
        def _():
            pltpu.make_async_copy(wv.at[d_rows], w_buf.at[slot], w_sem.at[slot]).start()

        @pl.when((s >= n_chunk) & (s < 3 * n_chunk))
        def _():
            tile = tile_of(s // n_chunk - 1)
            pltpu.make_async_copy(
                wq.at[d_rows, pl.ds(al(tile * tile_heads, tile_heads), tile_heads), :],
                w_buf.at[slot], w_sem.at[slot]).start()

    def w_wait(s):
        slot = lax.rem(s, DEPTH)
        pltpu.make_async_copy(wk.at[pl.ds(0, D_CHUNK)], w_buf.at[slot], w_sem.at[slot]).wait()

    for n in range(WO_DEPTH - 1):
        wo_copy(jnp.int32(n)).start()
    for s in range(DEPTH - 1):
        w_start(jnp.int32(s))

    my_low = al(core * seg, seg)
    my_high = al(rows + (1 - core) * seg, seg)
    for ref, stack in ((dy_ref, dys), (x_ref, xs)):
        stack[pl.ds(my_low, seg), :] = ref[:seg, :]
        stack[pl.ds(my_high, seg), :] = ref[seg:, :]
    dkv_acc[...] = jnp.zeros_like(dkv_acc)
    meet_group(n_dev)
    swaps = []
    for k, (ref, stack) in enumerate(((dy_ref, dys), (x_ref, xs))):
        swaps.append(rcopy(ref.at[pl.ds(0, seg)], stack.at[pl.ds(my_low, seg)],
                           x_send.at[k, 0], x_recv.at[k, 0], sib))
        swaps.append(rcopy(ref.at[pl.ds(seg, seg)], stack.at[pl.ds(my_high, seg)],
                           x_send.at[k, 1], x_recv.at[k, 1], sib))
    for swap in swaps:
        swap.start()
    swaps[0].wait()
    swaps[1].wait()

    def each(lo, hi, ship, act):
        def step(n, carry):
            ship(n, act)
            return carry
        lax.fori_loop(lo, hi, step, 0)

    def do_ship(n, act):
        dest = dest_of(n)
        for k, at in enumerate((low_at, high_at)):
            act(dest == me, st_do.at[n, pl.ds(k * rows, rows), :], do_all.at[pl.ds(at, rows), :],
                do_send.at[n, k], do_recv.at[chip, k], dest)

    def do_loop(lo, hi, send):
        def do_step(n, carry):
            @pl.when(n + WO_DEPTH - 1 < n_dest)
            def _():
                wo_copy(n + WO_DEPTH - 1).start()
            wo_copy(n).wait()

            if send:
                @pl.when(n > lo)
                def _():
                    do_ship(n - 1, ship_start)
            st_do[n] = lax.dot_general(dys[...], wo_buf[lax.rem(n, WO_DEPTH)], CONTRACT_LAST,
                                       preferred_element_type=F32).astype(BF16)
            return carry
        lax.fori_loop(lo, hi, do_step, 0)

    do_loop(0, DO_FIRST, True)
    swaps[2].wait()
    swaps[3].wait()

    def w2_copy(s):
        part = lax.rem(s, n_chunk)
        kind = s // n_chunk
        group = jnp.where(kind == 0, 0, 1 + lax.rem(kind - 1 + chip // 2, 2))
        slot = lax.rem(s, W2_DEPTH)
        return pltpu.make_async_copy(w2_buf.at[slot], w2_all.at[group * n_chunk + part], w2_sem.at[slot])

    def w_step(s, first):
        w_start(s + DEPTH - 1)
        w_wait(s)

        @pl.when(s >= 1)
        def _():
            w2_copy(s - 1).start()

        @pl.when(s >= W2_DEPTH)
        def _():
            w2_copy(s - W2_DEPTH).wait()
        part = lax.rem(s, n_chunk)
        w_tile = w_buf[lax.rem(s, DEPTH)].reshape(D_CHUNK, tile_w)
        w2_buf[lax.rem(s, W2_DEPTH)] = w_tile
        add = jnp.dot(xs[:, pl.ds(al(part * D_CHUNK, D_CHUNK), D_CHUNK)], w_tile,
                      preferred_element_type=F32)
        p_acc[...] = add if first else p_acc[...] + add

    def w_loop(lo, hi):
        def body(s, carry):
            w_step(s, False)
            return carry
        lax.fori_loop(lo, hi, body, 0)

    def kv_ship(n, act):
        dest_chip = lax.rem(n + chip, n_chip)
        dest = 2 * dest_chip + core
        lanes = pl.ds(al(dest_chip * head, head), head)
        for k, at in enumerate((low_at, high_at)):
            act(dest == me, st_kv.at[pl.ds(k * rows, rows), lanes], kv_all.at[core, pl.ds(at, rows), :],
                kv_send.at[dest_chip, k], kv_recv.at[chip, k], dest)

    def q_ship(n, act):
        t = n // 4
        dest = 4 * tile_of(t) + lax.rem(n + 2 * chip, 4)
        lanes = pl.ds(al(lax.rem(dest, 4) * wide, wide), wide)
        for k, at in enumerate((low_at, high_at)):
            act(dest == me, st_q.at[t, pl.ds(k * rows, rows), lanes], q_all.at[pl.ds(at, rows), :],
                q_send.at[n, k], q_recv.at[chip, k], dest)

    w_step(jnp.int32(0), True)
    do_ship(jnp.int32(DO_FIRST - 1), ship_start)
    w_loop(1, n_chunk)
    st_kv[...] = p_acc[...].astype(BF16)
    w_step(jnp.int32(n_chunk), True)
    each(0, n_chip, kv_ship, ship_start)
    w_loop(n_chunk + 1, 2 * n_chunk)
    st_q[0] = p_acc[...].astype(BF16)
    w_step(jnp.int32(2 * n_chunk), True)
    each(0, 4, q_ship, ship_start)
    w_loop(2 * n_chunk + 1, 3 * n_chunk)
    st_q[1] = p_acc[...].astype(BF16)
    w2_copy(jnp.int32(3 * n_chunk - 1)).start()

    def kv_arrive(src_chip, carry):
        @pl.when(src_chip != chip)
        def _():
            for k in range(2):
                rcopy(st_kv.at[pl.ds(0, rows), pl.ds(0, head)], kv_all.at[core, pl.ds(0, rows), :],
                      kv_send.at[0, k], kv_recv.at[src_chip, k], sib).wait_recv()
        return carry

    do_loop(DO_FIRST, DO_FIRST + 1, False)
    each(4, 8, q_ship, ship_start)
    do_loop(DO_FIRST + 1, n_dest, False)
    for k in range(W2_DEPTH):
        w2_copy(jnp.int32(3 * n_chunk - W2_DEPTH + k)).wait()
    lax.fori_loop(0, n_chip, kv_arrive, 0)
    each(0, n_chip, kv_ship, ship_wait)
    relay = rcopy(kv_all.at[core], kv_all.at[core], rel_send, rel_recv, sib)
    relay.start()
    rcopy(kv_all.at[core], kv_all.at[1 - core], rel_send, rel_recv, sib).wait_recv()
    relay.wait_send()
    k_t[...] = kv_all[0].T
    v_t[...] = kv_all[1].T
    each(0, 4, q_ship, ship_wait)
    each(DO_FIRST, 4, do_ship, ship_start)

    def chunks_of(qb):
        cuts = list(range(0, qb * BQ, BK)) + [qb * BQ, (qb + 1) * BQ]
        return [slice(lo, hi) for lo, hi in zip(cuts[:-1], cuts[1:])]

    def s_at(ks):
        return slice(ks.start // BQ, ks.stop // BQ)

    def p_rows(qb, ks):
        base = BQ * (qb * (qb + 1) // 2)
        return slice(base + ks.start, base + ks.stop)

    def forward(qb):
        q_rows = slice(qb * BQ, (qb + 1) * BQ)
        q = [q_all[q_rows, h * head:(h + 1) * head] for h in range(heads)]
        chunks = chunks_of(qb)
        tops = [[] for _ in range(heads)]
        sums = [[] for _ in range(heads)]
        for ks in chunks:
            k_blk = kv_all[0, ks, :]
            for h in range(heads):
                s = lax.dot_general(k_blk, q[h], CONTRACT_LAST, preferred_element_type=F32)
                if ks.start == qb * BQ:
                    k_pos = lax.broadcasted_iota(jnp.int32, (BQ, BQ), 0)
                    q_pos = lax.broadcasted_iota(jnp.int32, (BQ, BQ), 1)
                    s = jnp.where(k_pos <= q_pos, s, -jnp.inf)
                top = jnp.max(s, axis=0, keepdims=True) * to_log2
                e = jnp.exp2(s * to_log2 - top)
                acc[s_at(ks), h * BQ:(h + 1) * BQ, :] = e.reshape(-1, BQ, BQ)
                tops[h].append(top)
                sums[h].append(jnp.sum(e, axis=0, keepdims=True))
        for h in range(heads):
            top = functools.reduce(jnp.maximum, tops[h])
            lift = [jnp.exp2(t - top) for t in tops[h]]
            inv = 1.0 / sum(a * b for a, b in zip(lift, sums[h]))
            o_t = None
            for ks, up in zip(chunks, lift):
                p = (acc[s_at(ks), h * BQ:(h + 1) * BQ, :].reshape(-1, BQ) * (up * inv)).astype(BF16)
                p_all[h, p_rows(qb, ks), :] = p
                part = jnp.dot(v_t[:, ks], p, preferred_element_type=F32)
                o_t = part if o_t is None else o_t + part
            o_all[h, :, q_rows] = o_t.astype(BF16)

    def backward(qb):
        q_rows = slice(qb * BQ, (qb + 1) * BQ)
        q = [q_all[q_rows, h * head:(h + 1) * head] for h in range(heads)]
        do = [do_all[q_rows, h * head:(h + 1) * head] for h in range(heads)]
        delta = [jnp.sum(do[h].astype(F32).T * o_all[h, :, q_rows].astype(F32), axis=0, keepdims=True)
                 for h in range(heads)]
        dq_t = [None] * heads
        for ks in chunks_of(qb):
            v_blk = kv_all[1, ks, :]
            dk = dv = None
            for h in range(heads):
                p = p_all[h, p_rows(qb, ks), :]
                dp = lax.dot_general(v_blk, do[h], CONTRACT_LAST, preferred_element_type=F32)
                ds = (p.astype(F32) * (dp - delta[h])).astype(BF16)
                part = jnp.dot(k_t[:, ks], ds, preferred_element_type=F32)
                dq_t[h] = part if dq_t[h] is None else dq_t[h] + part
                dk_h = jnp.dot(ds, q[h], preferred_element_type=F32)
                dv_h = jnp.dot(p, do[h], preferred_element_type=F32)
                dk = dk_h if dk is None else dk + dk_h
                dv = dv_h if dv is None else dv + dv_h
            dkv_acc[0, ks, :] += dk
            dkv_acc[1, ks, :] += dv
        for h in range(heads):
            dq_st[q_rows, h * head:(h + 1) * head] = (dq_t[h] * scale).T.astype(BF16)

    def block_at(step):
        side = lax.rem(lax.rem(chip, 4) // 2 + step // 4, 2)
        spot = lax.rem(step + lax.rem(chip, 2) + 2 * (chip // 4), 4)
        return jnp.where(spot < 2, 2 * spot + side, 11 - 2 * spot - side)

    def home_of(block):
        return jnp.where(block < n_chip, block, 2 * n_chip - 1 - block)

    def ahead(step, carry):
        qb = block_at(step)

        @pl.when(step == n_block // 2)
        def _():
            each(4, 8, q_ship, ship_wait)
            each(4, n_dest, do_ship, ship_start)
        for i in range(per):
            block = qb * per + i
            home = home_of(block)

            @pl.when(2 * home + my_src_core != me)
            def _():
                rcopy(st_do.at[0, pl.ds(0, rows), :], q_all.at[pl.ds(0, rows), :],
                      q_send.at[0, 0], q_recv.at[home, block // n_chip], sib).wait_recv()
        for which in range(n_block):
            @pl.when(qb == which)
            def _():
                forward(which)
        return carry

    lax.fori_loop(0, n_block, ahead, 0)

    src_slot = lax.rem(me, n_dest)

    def dq_ship(block, act):
        k = block // n_chip
        dest = 2 * home_of(block) + my_src_core
        act(dest == me, dq_st.at[pl.ds(al(block * rows, rows), rows), :],
            dq_in.at[src_slot // 4, pl.ds(al(k * rows, rows), rows), pl.ds(al(lax.rem(src_slot, 4) * wide, wide), wide)],
            dq_send.at[block], dq_recv.at[src_slot, k], dest)

    def do_done(n, carry):
        @pl.when(dest_of(n) == me)
        def _():
            do_ship(n, ship_wait)
        return carry

    lax.fori_loop(0, n_dest, do_done, 0)

    def back(step, carry):
        qb = block_at(step)
        for i in range(per):
            block = qb * per + i
            home = home_of(block)

            @pl.when(2 * home + my_src_core != me)
            def _():
                rcopy(st_do.at[0, pl.ds(0, rows), :], do_all.at[pl.ds(0, rows), :],
                      do_send.at[0, 0], do_recv.at[home, block // n_chip], sib).wait_recv()
        for which in range(n_block):
            @pl.when(qb == which)
            def _():
                backward(which)
        for i in range(per):
            dq_ship(qb * per + i, ship_start)
        return carry

    lax.fori_loop(0, n_block, back, 0)
    swap = rcopy(dkv_acc.at[1 - core], dkv_far, red_send, red_recv, sib)
    swap.start()

    def stream_copy(u):
        group = jnp.where(u < 2 * n_chunk, 1 + lax.rem(u, 2), 0)
        part = jnp.where(u < 2 * n_chunk, u // 2, u - 2 * n_chunk)
        slot = lax.rem(u, W2_DEPTH)
        return pltpu.make_async_copy(w2_all.at[group * n_chunk + part], w2_buf.at[slot], w2_sem.at[slot])

    for u in range(W2_DEPTH - 1):
        stream_copy(jnp.int32(u)).start()

    def do_sent(n, carry):
        @pl.when(dest_of(n) != me)
        def _():
            do_ship(n, ship_wait)
        return carry

    lax.fori_loop(0, n_dest, do_sent, 0)

    def dkv_ship(n, act):
        dest_chip = lax.rem(chip + n, n_chip)
        dest = 2 * dest_chip + core
        for k in range(2):
            block = dest_chip if k == 0 else 2 * n_chip - 1 - dest_chip
            act(dest == me, dkv_st.at[pl.ds(al(block * rows, rows), rows), :],
                dkv_in.at[pl.ds(k * rows, rows), pl.ds(al(chip * head, head), head)],
                dkv_send.at[n, k], dkv_recv.at[chip, k], dest)

    swap.wait()
    factor = jnp.where(core == 0, scale, 1.0).astype(F32)
    dkv_st[...] = ((dkv_acc[core] + dkv_far[...]) * factor).astype(BF16)
    each(0, n_chip, dkv_ship, ship_start)
    each(0, n_block * per, dq_ship, ship_wait)

    def dq_arrive(src, carry):
        @pl.when(n_dest * core + src != me)
        def _():
            for k in range(2):
                rcopy(dq_st.at[pl.ds(0, rows), :], dq_in.at[0, pl.ds(0, rows), pl.ds(0, wide)],
                      dq_send.at[0], dq_recv.at[src, k], sib).wait_recv()
        return carry

    lax.fori_loop(0, n_dest, dq_arrive, 0)

    def by_token(x):
        return jnp.concatenate([x[:seg], x[3 * seg:], x[seg:3 * seg]], axis=0).T

    def matmul(group, u):
        @pl.when(u + W2_DEPTH - 1 < 3 * n_chunk)
        def _():
            stream_copy(u + W2_DEPTH - 1).start()
        stream_copy(u).wait()
        return jnp.dot(w2_buf[lax.rem(u, W2_DEPTH)], grads_t[group], preferred_element_type=F32)

    grads_t[0] = by_token(dq_in[0])
    grads_t[1] = by_token(dq_in[1])

    def first_pass(part, carry):
        acc[part] = matmul(0, 2 * part)
        acc[part] += matmul(1, 2 * part + 1)
        return carry

    lax.fori_loop(0, n_chunk, first_pass, 0)
    each(0, n_chip, dkv_ship, ship_wait)

    def dkv_arrive(src_chip, carry):
        @pl.when(src_chip != chip)
        def _():
            for k in range(2):
                rcopy(dkv_st.at[pl.ds(0, rows), :], dkv_in.at[pl.ds(0, rows), pl.ds(0, head)],
                      dkv_send.at[0, k], dkv_recv.at[src_chip, k], sib).wait_recv()
        return carry

    lax.fori_loop(0, n_chip, dkv_arrive, 0)

    grads_t[2] = by_token(dkv_in[...])
    my_lanes = pl.ds(al(core * rows, rows), rows)
    sib_lanes = pl.ds(al((1 - core) * rows, rows), rows)

    def far_copy(part):
        return rcopy(acc.at[part, :, sib_lanes], far.at[part], far_send.at[part], far_recv.at[part], sib)

    def last_pass(part, carry):
        acc[part] += matmul(2, 2 * n_chunk + part)

        @pl.when(part > 0)
        def _():
            far_copy(part - 1).start()
        return carry

    lax.fori_loop(0, n_chunk, last_pass, 0)
    far_copy(n_chunk - 1).start()

    def finish(part, carry):
        far_copy(part).wait()
        dx_ref[:, pl.ds(al(part * D_CHUNK, D_CHUNK), D_CHUNK)] = (acc[part, :, my_lanes] + far[part]).astype(BF16).T
        return carry

    lax.fori_loop(0, n_chunk, finish, 0)


def solution(mesh):
    n_dev = mesh.shape["cp"]
    n_chip = n_dev // 2
    row_spec = P(("dp", "cp"), None)
    any_spec = pl.BlockSpec(memory_space=pl.ANY)
    vmem_spec = pl.BlockSpec(memory_space=pltpu.VMEM)
    dma = pltpu.SemaphoreType.DMA

    def device_fn(x_in, d_y, w_q, w_k, w_v, w_o):
        rows, d_model = x_in.shape
        q_heads, head = w_q.shape[1], w_q.shape[2]
        kv_heads = w_k.shape[1]
        seq = rows * n_dev
        scale = head ** -0.5
        wide = q_heads // n_dev * head
        tile_w = kv_heads * head
        n_chunk = d_model // D_CHUNK
        wo_flat = w_o.reshape(q_heads * head, d_model)
        params = functools.partial(pltpu.CompilerParams, vmem_limit_bytes=VMEM_LIMIT)
        tri = (seq // BQ) * (seq // BQ + 1) // 2 * BQ
        return pl.pallas_call(
            functools.partial(fused_kernel, n_dev, scale),
            out_shape=(jax.ShapeDtypeStruct((rows, d_model), BF16),
                       jax.ShapeDtypeStruct((3 * n_chunk, D_CHUNK, tile_w), BF16)),
            in_specs=[vmem_spec, vmem_spec, any_spec, any_spec, any_spec, any_spec],
            out_specs=(vmem_spec, any_spec),
            scratch_shapes=[
                pltpu.VMEM((2 * rows, d_model), BF16),
                pltpu.VMEM((2 * rows, d_model), BF16),
                pltpu.VMEM((WO_DEPTH, wide, d_model), BF16),
                pltpu.VMEM((DEPTH, D_CHUNK, kv_heads, head), BF16),
                pltpu.VMEM((W2_DEPTH, D_CHUNK, tile_w), BF16),
                pltpu.VMEM((2 * rows, tile_w), F32),
                pltpu.VMEM((n_chip, 2 * rows, wide), BF16),
                pltpu.VMEM((2 * rows, tile_w), BF16),
                pltpu.VMEM((2, 2 * rows, tile_w), BF16),
                pltpu.VMEM((seq, wide), BF16),
                pltpu.VMEM((seq, wide), BF16),
                pltpu.VMEM((2, seq, head), BF16),
                pltpu.VMEM((head, seq), BF16),
                pltpu.VMEM((head, seq), BF16),
                pltpu.VMEM((wide // head, tri, BQ), BF16),
                pltpu.VMEM((wide // head, head, seq), BF16),
                pltpu.VMEM((seq, wide), BF16),
                pltpu.VMEM((2, seq, head), F32),
                pltpu.VMEM((2, 2 * rows, tile_w), BF16),
                pltpu.VMEM((2 * rows, tile_w), BF16),
                pltpu.VMEM((seq, head), F32),
                pltpu.VMEM((seq, head), BF16),
                pltpu.VMEM((3, tile_w, 2 * rows), BF16),
                pltpu.VMEM((n_chunk, D_CHUNK, 2 * rows), F32),
                pltpu.VMEM((n_chunk, D_CHUNK, rows), F32),
                dma((WO_DEPTH,)), dma((DEPTH,)), dma((W2_DEPTH,)), dma((2, 2)), dma((2, 2)),
                dma((n_chip, 2)), dma((n_chip, 2)), dma((n_chip, 2)), dma((n_chip, 2)),
                dma((n_chip, 2)), dma((n_chip, 2)), dma, dma,
                dma((seq // rows,)), dma((n_chip, 2)), dma((n_chip, 2)), dma((n_chip, 2)),
                dma((n_chunk,)), dma((n_chunk,)), dma, dma,
            ],
            compiler_params=params(collective_id=0, has_side_effects=True),
            name="fused",
        )(x_in, d_y, w_q, w_k, w_v, wo_flat)[0]

    return jax.shard_map(device_fn, mesh=mesh, in_specs=(row_spec, row_spec, P(), P(), P(), P()),
                         out_specs=row_spec, check_vma=False)
```

```python
import functools

import jax
import jax.numpy as jnp
from jax import lax
from jax.experimental import pallas as pl
from jax.experimental.pallas import tpu as pltpu
from jax.sharding import PartitionSpec as P

MESH = pl.DeviceIdType.MESH
BF16 = jnp.bfloat16
F32 = jnp.float32
CONTRACT_LAST = (((1,), (1,)), ((), ()))
DEPTH = 4
W2_DEPTH = 8
WO_DEPTH = 2
D_CHUNK = 512
BQ = 256
BK = 512
DO_FIRST = 2
VMEM_LIMIT = 62 * 2 ** 20


def place():
    me = lax.axis_index("cp")
    chip = me // 2
    core = me % 2
    return me, chip, core, me + 1 - 2 * core


def meet_group(n_dev):
    me = lax.axis_index("cp")
    barrier = pltpu.get_barrier_semaphore()

    def greet(step, carry):
        other = lax.rem(me + step, n_dev)
        pl.semaphore_signal(barrier, inc=1, device_id={"cp": other}, device_id_type=MESH)
        return carry

    lax.fori_loop(1, n_dev, greet, 0)
    pl.semaphore_wait(barrier, n_dev - 1)


def rcopy(src, dst, send_sem, recv_sem, dev):
    return pltpu.make_async_remote_copy(
        src_ref=src, dst_ref=dst, send_sem=send_sem, recv_sem=recv_sem,
        device_id={"cp": dev}, device_id_type=MESH)


def al(value, step):
    return pl.multiple_of(value, step)


def ship_start(is_me, src, dst, send_sem, recv_sem, dev):
    @pl.when(is_me)
    def _():
        pltpu.make_async_copy(src, dst, send_sem).start()

    @pl.when(jnp.logical_not(is_me))
    def _():
        rcopy(src, dst, send_sem, recv_sem, dev).start()


def ship_wait(is_me, src, dst, send_sem, recv_sem, dev):
    @pl.when(is_me)
    def _():
        pltpu.make_async_copy(src, dst, send_sem).wait()

    @pl.when(jnp.logical_not(is_me))
    def _():
        rcopy(src, dst, send_sem, recv_sem, dev).wait_send()


def fused_kernel(n_dev, scale, x_ref, dy_ref, wq, wk, wv, wo, dx_ref, w2_all,
                 xs, dys, wo_buf, w_buf, w2_buf, p_acc, st_do, st_kv, st_q,
                 q_all, do_all, kv_all, k_t, v_t, p_all, o_all, dq_st, dkv_acc,
                 dq_in, dkv_in, dkv_far, dkv_st, grads_t, acc, far,
                 wo_sem, w_sem, w2_sem, x_send, x_recv, do_send, do_recv,
                 kv_send, kv_recv, q_send, q_recv, rel_send, rel_recv,
                 dq_send, dq_recv, dkv_send, dkv_recv, far_send, far_recv, red_send, red_recv):
    me, chip, core, sib = place()
    n_chip = n_dev // 2
    rows, d_model = x_ref.shape
    seg = rows // 2
    seq, wide = q_all.shape
    head = kv_all.shape[2]
    heads = wide // head
    tile_w = p_acc.shape[1]
    n_chunk = d_model // D_CHUNK
    n_dest = n_dev // 2
    tile_heads = w_buf.shape[2]
    my_src_core = chip // (n_chip // 2)
    low_at = al(chip * rows, rows)
    high_at = al((2 * n_chip - 1 - chip) * rows, rows)
    n_block = seq // BQ
    per = BQ // rows
    to_log2 = scale * 1.4426950408889634

    def dest_of(n):
        spot, step = lax.rem(chip, 4), n // 2
        flip = 2 * lax.rem(spot // 2 + step // 2, 2) + lax.rem(spot + step, 2)
        return n_dest * core + 2 * flip + lax.rem(n, 2)

    def wo_copy(n):
        return pltpu.make_async_copy(
            wo.at[pl.ds(al(dest_of(n) * wide, wide), wide), :], wo_buf.at[lax.rem(n, WO_DEPTH)],
            wo_sem.at[lax.rem(n, WO_DEPTH)])

    def tile_of(t):
        return 2 * core + lax.rem(t + chip // 2, 2)

    def w_start(s):
        slot = lax.rem(s, DEPTH)
        part = lax.rem(s, n_chunk)
        d_rows = pl.ds(al(part * D_CHUNK, D_CHUNK), D_CHUNK)

        @pl.when((s < n_chunk) & (core == 0))
        def _():
            pltpu.make_async_copy(wk.at[d_rows], w_buf.at[slot], w_sem.at[slot]).start()

        @pl.when((s < n_chunk) & (core == 1))
        def _():
            pltpu.make_async_copy(wv.at[d_rows], w_buf.at[slot], w_sem.at[slot]).start()

        @pl.when((s >= n_chunk) & (s < 3 * n_chunk))
        def _():
            tile = tile_of(s // n_chunk - 1)
            pltpu.make_async_copy(
                wq.at[d_rows, pl.ds(al(tile * tile_heads, tile_heads), tile_heads), :],
                w_buf.at[slot], w_sem.at[slot]).start()

    def w_wait(s):
        slot = lax.rem(s, DEPTH)
        pltpu.make_async_copy(wk.at[pl.ds(0, D_CHUNK)], w_buf.at[slot], w_sem.at[slot]).wait()

    for n in range(WO_DEPTH - 1):
        wo_copy(jnp.int32(n)).start()
    for s in range(DEPTH - 1):
        w_start(jnp.int32(s))

    my_low = al(core * seg, seg)
    my_high = al(rows + (1 - core) * seg, seg)
    for ref, stack in ((dy_ref, dys), (x_ref, xs)):
        stack[pl.ds(my_low, seg), :] = ref[:seg, :]
        stack[pl.ds(my_high, seg), :] = ref[seg:, :]
    dkv_acc[...] = jnp.zeros_like(dkv_acc)
    meet_group(n_dev)
    swaps = []
    for k, (ref, stack) in enumerate(((dy_ref, dys), (x_ref, xs))):
        swaps.append(rcopy(ref.at[pl.ds(0, seg)], stack.at[pl.ds(my_low, seg)],
                           x_send.at[k, 0], x_recv.at[k, 0], sib))
        swaps.append(rcopy(ref.at[pl.ds(seg, seg)], stack.at[pl.ds(my_high, seg)],
                           x_send.at[k, 1], x_recv.at[k, 1], sib))
    for swap in swaps:
        swap.start()
    swaps[0].wait()
    swaps[1].wait()

    def each(lo, hi, ship, act):
        def step(n, carry):
            ship(n, act)
            return carry
        lax.fori_loop(lo, hi, step, 0)

    def do_ship(n, act):
        dest = dest_of(n)
        for k, at in enumerate((low_at, high_at)):
            act(dest == me, st_do.at[n, pl.ds(k * rows, rows), :], do_all.at[pl.ds(at, rows), :],
                do_send.at[n, k], do_recv.at[chip, k], dest)

    def do_loop(lo, hi, send):
        def do_step(n, carry):
            @pl.when(n + WO_DEPTH - 1 < n_dest)
            def _():
                wo_copy(n + WO_DEPTH - 1).start()
            wo_copy(n).wait()

            if send:
                @pl.when(n > lo)
                def _():
                    do_ship(n - 1, ship_start)
            st_do[n] = lax.dot_general(dys[...], wo_buf[lax.rem(n, WO_DEPTH)], CONTRACT_LAST,
                                       preferred_element_type=F32).astype(BF16)
            return carry
        lax.fori_loop(lo, hi, do_step, 0)

    do_loop(0, DO_FIRST, True)
    swaps[2].wait()
    swaps[3].wait()

    def w2_copy(s):
        part = lax.rem(s, n_chunk)
        kind = s // n_chunk
        group = jnp.where(kind == 0, 0, 1 + lax.rem(kind - 1 + chip // 2, 2))
        slot = lax.rem(s, W2_DEPTH)
        return pltpu.make_async_copy(w2_buf.at[slot], w2_all.at[group * n_chunk + part], w2_sem.at[slot])

    def w_step(s, first):
        w_start(s + DEPTH - 1)
        w_wait(s)

        @pl.when(s >= 1)
        def _():
            w2_copy(s - 1).start()

        @pl.when(s >= W2_DEPTH)
        def _():
            w2_copy(s - W2_DEPTH).wait()
        part = lax.rem(s, n_chunk)
        w_tile = w_buf[lax.rem(s, DEPTH)].reshape(D_CHUNK, tile_w)
        w2_buf[lax.rem(s, W2_DEPTH)] = w_tile
        add = jnp.dot(xs[:, pl.ds(al(part * D_CHUNK, D_CHUNK), D_CHUNK)], w_tile,
                      preferred_element_type=F32)
        p_acc[...] = add if first else p_acc[...] + add

    def w_loop(lo, hi):
        def body(s, carry):
            w_step(s, False)
            return carry
        lax.fori_loop(lo, hi, body, 0)

    def kv_ship(n, act):
        dest_chip = lax.rem(n + chip, n_chip)
        dest = 2 * dest_chip + core
        lanes = pl.ds(al(dest_chip * head, head), head)
        for k, at in enumerate((low_at, high_at)):
            act(dest == me, st_kv.at[pl.ds(k * rows, rows), lanes], kv_all.at[core, pl.ds(at, rows), :],
                kv_send.at[dest_chip, k], kv_recv.at[chip, k], dest)

    def q_ship(n, act):
        t = n // 4
        dest = 4 * tile_of(t) + lax.rem(n + 2 * chip, 4)
        lanes = pl.ds(al(lax.rem(dest, 4) * wide, wide), wide)
        for k, at in enumerate((low_at, high_at)):
            act(dest == me, st_q.at[t, pl.ds(k * rows, rows), lanes], q_all.at[pl.ds(at, rows), :],
                q_send.at[n, k], q_recv.at[chip, k], dest)

    w_step(jnp.int32(0), True)
    do_ship(jnp.int32(DO_FIRST - 1), ship_start)
    w_loop(1, n_chunk)
    st_kv[...] = p_acc[...].astype(BF16)
    w_step(jnp.int32(n_chunk), True)
    each(0, n_chip, kv_ship, ship_start)
    w_loop(n_chunk + 1, 2 * n_chunk)
    st_q[0] = p_acc[...].astype(BF16)
    w_step(jnp.int32(2 * n_chunk), True)
    each(0, 4, q_ship, ship_start)
    w_loop(2 * n_chunk + 1, 3 * n_chunk)
    st_q[1] = p_acc[...].astype(BF16)
    w2_copy(jnp.int32(3 * n_chunk - 1)).start()

    def kv_arrive(src_chip, carry):
        @pl.when(src_chip != chip)
        def _():
            for k in range(2):
                rcopy(st_kv.at[pl.ds(0, rows), pl.ds(0, head)], kv_all.at[core, pl.ds(0, rows), :],
                      kv_send.at[0, k], kv_recv.at[src_chip, k], sib).wait_recv()
        return carry

    do_loop(DO_FIRST, DO_FIRST + 1, False)
    each(4, 8, q_ship, ship_start)
    do_loop(DO_FIRST + 1, n_dest, False)
    for k in range(W2_DEPTH):
        w2_copy(jnp.int32(3 * n_chunk - W2_DEPTH + k)).wait()
    lax.fori_loop(0, n_chip, kv_arrive, 0)
    each(0, n_chip, kv_ship, ship_wait)
    relay = rcopy(kv_all.at[core], kv_all.at[core], rel_send, rel_recv, sib)
    relay.start()
    rcopy(kv_all.at[core], kv_all.at[1 - core], rel_send, rel_recv, sib).wait_recv()
    relay.wait_send()
    k_t[...] = kv_all[0].T
    v_t[...] = kv_all[1].T
    each(0, 4, q_ship, ship_wait)
    each(DO_FIRST, 4, do_ship, ship_start)

    def chunks_of(qb):
        cuts = list(range(0, qb * BQ, BK)) + [qb * BQ, (qb + 1) * BQ]
        return [slice(lo, hi) for lo, hi in zip(cuts[:-1], cuts[1:])]

    def s_at(ks):
        return slice(ks.start // BQ, ks.stop // BQ)

    def p_rows(qb, ks):
        base = BQ * (qb * (qb + 1) // 2)
        return slice(base + ks.start, base + ks.stop)

    def forward(qb):
        q_rows = slice(qb * BQ, (qb + 1) * BQ)
        q = [q_all[q_rows, h * head:(h + 1) * head] for h in range(heads)]
        chunks = chunks_of(qb)
        tops = [[] for _ in range(heads)]
        sums = [[] for _ in range(heads)]
        for ks in chunks:
            k_blk = kv_all[0, ks, :]
            for h in range(heads):
                s = lax.dot_general(k_blk, q[h], CONTRACT_LAST, preferred_element_type=F32)
                if ks.start == qb * BQ:
                    k_pos = lax.broadcasted_iota(jnp.int32, (BQ, BQ), 0)
                    q_pos = lax.broadcasted_iota(jnp.int32, (BQ, BQ), 1)
                    s = jnp.where(k_pos <= q_pos, s, -jnp.inf)
                top = jnp.max(s, axis=0, keepdims=True) * to_log2
                e = jnp.exp2(s * to_log2 - top)
                acc[s_at(ks), h * BQ:(h + 1) * BQ, :] = e.reshape(-1, BQ, BQ)
                tops[h].append(top)
                sums[h].append(jnp.sum(e, axis=0, keepdims=True))
        for h in range(heads):
            top = functools.reduce(jnp.maximum, tops[h])
            lift = [jnp.exp2(t - top) for t in tops[h]]
            inv = 1.0 / sum(a * b for a, b in zip(lift, sums[h]))
            o_t = None
            for ks, up in zip(chunks, lift):
                p = (acc[s_at(ks), h * BQ:(h + 1) * BQ, :].reshape(-1, BQ) * (up * inv)).astype(BF16)
                p_all[h, p_rows(qb, ks), :] = p
                part = jnp.dot(v_t[:, ks], p, preferred_element_type=F32)
                o_t = part if o_t is None else o_t + part
            o_all[h, :, q_rows] = o_t.astype(BF16)

    def backward(qb):
        q_rows = slice(qb * BQ, (qb + 1) * BQ)
        q = [q_all[q_rows, h * head:(h + 1) * head] for h in range(heads)]
        do = [do_all[q_rows, h * head:(h + 1) * head] for h in range(heads)]
        delta = [jnp.sum(do[h].astype(F32).T * o_all[h, :, q_rows].astype(F32), axis=0, keepdims=True)
                 for h in range(heads)]
        dq_t = [None] * heads
        for ks in chunks_of(qb):
            v_blk = kv_all[1, ks, :]
            dk = dv = None
            for h in range(heads):
                p = p_all[h, p_rows(qb, ks), :]
                dp = lax.dot_general(v_blk, do[h], CONTRACT_LAST, preferred_element_type=F32)
                ds = (p.astype(F32) * (dp - delta[h])).astype(BF16)
                part = jnp.dot(k_t[:, ks], ds, preferred_element_type=F32)
                dq_t[h] = part if dq_t[h] is None else dq_t[h] + part
                dk_h = jnp.dot(ds, q[h], preferred_element_type=F32)
                dv_h = jnp.dot(p, do[h], preferred_element_type=F32)
                dk = dk_h if dk is None else dk + dk_h
                dv = dv_h if dv is None else dv + dv_h
            dkv_acc[0, ks, :] += dk
            dkv_acc[1, ks, :] += dv
        for h in range(heads):
            dq_st[q_rows, h * head:(h + 1) * head] = (dq_t[h] * scale).T.astype(BF16)

    def block_at(step):
        side = lax.rem(lax.rem(chip, 4) // 2 + step // 4, 2)
        spot = lax.rem(step + lax.rem(chip, 2) + 2 * (chip // 4), 4)
        return jnp.where(spot < 2, 2 * spot + side, 11 - 2 * spot - side)

    def home_of(block):
        return jnp.where(block < n_chip, block, 2 * n_chip - 1 - block)

    def ahead(step, carry):
        qb = block_at(step)

        @pl.when(step == n_block // 2)
        def _():
            each(4, 8, q_ship, ship_wait)
            each(4, n_dest, do_ship, ship_start)
        for i in range(per):
            block = qb * per + i
            home = home_of(block)

            @pl.when(2 * home + my_src_core != me)
            def _():
                rcopy(st_do.at[0, pl.ds(0, rows), :], q_all.at[pl.ds(0, rows), :],
                      q_send.at[0, 0], q_recv.at[home, block // n_chip], sib).wait_recv()
        for which in range(n_block):
            @pl.when(qb == which)
            def _():
                forward(which)
        return carry

    lax.fori_loop(0, n_block, ahead, 0)

    src_slot = lax.rem(me, n_dest)

    def dq_ship(block, act):
        k = block // n_chip
        dest = 2 * home_of(block) + my_src_core
        act(dest == me, dq_st.at[pl.ds(al(block * rows, rows), rows), :],
            dq_in.at[src_slot // 4, pl.ds(al(k * rows, rows), rows), pl.ds(al(lax.rem(src_slot, 4) * wide, wide), wide)],
            dq_send.at[block], dq_recv.at[src_slot, k], dest)

    def do_done(n, carry):
        @pl.when(dest_of(n) == me)
        def _():
            do_ship(n, ship_wait)
        return carry

    lax.fori_loop(0, n_dest, do_done, 0)

    def back(step, carry):
        qb = block_at(step)
        for i in range(per):
            block = qb * per + i
            home = home_of(block)

            @pl.when(2 * home + my_src_core != me)
            def _():
                rcopy(st_do.at[0, pl.ds(0, rows), :], do_all.at[pl.ds(0, rows), :],
                      do_send.at[0, 0], do_recv.at[home, block // n_chip], sib).wait_recv()
        for which in range(n_block):
            @pl.when(qb == which)
            def _():
                backward(which)
        for i in range(per):
            dq_ship(qb * per + i, ship_start)
        return carry

    lax.fori_loop(0, n_block, back, 0)
    swap = rcopy(dkv_acc.at[1 - core], dkv_far, red_send, red_recv, sib)
    swap.start()

    early = lax.rem(chip, 4) // 2
    n_pair = n_chunk // 2
    n_slot = W2_DEPTH // 2

    def stream_copy(u):
        turn = u // n_pair
        group = jnp.where(turn == 0, 1 + early, jnp.where(turn == 1, 2 - early, 0))
        part = group * n_chunk + 2 * lax.rem(u, n_pair)
        slot = lax.rem(u, n_slot)
        return pltpu.make_async_copy(w2_all.at[pl.ds(part, 2)], w2_buf.at[pl.ds(2 * slot, 2)], w2_sem.at[slot])

    for u in range(n_slot - 1):
        stream_copy(jnp.int32(u)).start()

    def do_sent(n, carry):
        @pl.when(dest_of(n) != me)
        def _():
            do_ship(n, ship_wait)
        return carry

    lax.fori_loop(0, n_dest, do_sent, 0)

    def dkv_ship(n, act):
        dest_chip = lax.rem(chip + n, n_chip)
        dest = 2 * dest_chip + core
        for k in range(2):
            block = dest_chip if k == 0 else 2 * n_chip - 1 - dest_chip
            act(dest == me, dkv_st.at[pl.ds(al(block * rows, rows), rows), :],
                dkv_in.at[pl.ds(k * rows, rows), pl.ds(al(chip * head, head), head)],
                dkv_send.at[n, k], dkv_recv.at[chip, k], dest)

    swap.wait()
    factor = jnp.where(core == 0, scale, 1.0).astype(F32)
    dkv_st[...] = ((dkv_acc[core] + dkv_far[...]) * factor).astype(BF16)
    each(0, n_chip, dkv_ship, ship_start)

    def dq_arrive(n, carry):
        src = lax.rem(4 * early + n, n_dest)

        @pl.when(n_dest * core + src != me)
        def _():
            for k in range(2):
                rcopy(dq_st.at[pl.ds(0, rows), :], dq_in.at[0, pl.ds(0, rows), pl.ds(0, wide)],
                      dq_send.at[0], dq_recv.at[src, k], sib).wait_recv()

        @pl.when(n_dest * core + src == me)
        def _():
            for k in range(2):
                dq_ship(jnp.where(k == 0, chip, 2 * n_chip - 1 - chip), ship_wait)
        return carry

    def by_token(x):
        return jnp.concatenate([x[:seg], x[3 * seg:], x[seg:3 * seg]], axis=0).T

    def matmul(group, u):
        @pl.when(u + n_slot - 1 < 3 * n_pair)
        def _():
            stream_copy(u + n_slot - 1).start()
        stream_copy(u).wait()
        pair = w2_buf[pl.ds(2 * lax.rem(u, n_slot), 2)].reshape(2 * D_CHUNK, tile_w)
        return jnp.dot(pair, grads_t[group], preferred_element_type=F32).reshape(2, D_CHUNK, 2 * rows)

    lax.fori_loop(0, n_dest // 2, dq_arrive, 0)
    grads_t[0] = by_token(dq_in[early])

    def early_pass(part, carry):
        acc[pl.ds(2 * part, 2)] = matmul(0, part)
        return carry

    lax.fori_loop(0, n_pair, early_pass, 0)
    lax.fori_loop(n_dest // 2, n_dest, dq_arrive, 0)
    grads_t[1] = by_token(dq_in[1 - early])

    def late_pass(part, carry):
        acc[pl.ds(2 * part, 2)] += matmul(1, n_pair + part)
        return carry

    lax.fori_loop(0, n_pair, late_pass, 0)

    def dq_sent(block, carry):
        @pl.when(2 * home_of(block) + my_src_core != me)
        def _():
            dq_ship(block, ship_wait)
        return carry

    lax.fori_loop(0, n_block * per, dq_sent, 0)
    each(0, n_chip, dkv_ship, ship_wait)

    def dkv_arrive(src_chip, carry):
        @pl.when(src_chip != chip)
        def _():
            for k in range(2):
                rcopy(dkv_st.at[pl.ds(0, rows), :], dkv_in.at[pl.ds(0, rows), pl.ds(0, head)],
                      dkv_send.at[0, k], dkv_recv.at[src_chip, k], sib).wait_recv()
        return carry

    lax.fori_loop(0, n_chip, dkv_arrive, 0)

    grads_t[2] = by_token(dkv_in[...])
    my_lanes = pl.ds(al(core * rows, rows), rows)
    sib_lanes = pl.ds(al((1 - core) * rows, rows), rows)

    def far_copy(part):
        two = pl.ds(2 * part, 2)
        return rcopy(acc.at[two, :, sib_lanes], far.at[two], far_send.at[part], far_recv.at[part], sib)

    def last_pass(part, carry):
        acc[pl.ds(2 * part, 2)] += matmul(2, 2 * n_pair + part)

        @pl.when(part > 0)
        def _():
            far_copy(part - 1).start()
        return carry

    lax.fori_loop(0, n_pair, last_pass, 0)
    far_copy(n_pair - 1).start()

    def finish(part, carry):
        far_copy(part).wait()
        for k in range(2):
            piece = 2 * part + k
            dx_ref[:, pl.ds(al(piece * D_CHUNK, D_CHUNK), D_CHUNK)] = (
                acc[piece, :, my_lanes] + far[piece]).astype(BF16).T
        return carry

    lax.fori_loop(0, n_pair, finish, 0)


def solution(mesh):
    n_dev = mesh.shape["cp"]
    n_chip = n_dev // 2
    row_spec = P(("dp", "cp"), None)
    any_spec = pl.BlockSpec(memory_space=pl.ANY)
    vmem_spec = pl.BlockSpec(memory_space=pltpu.VMEM)
    dma = pltpu.SemaphoreType.DMA

    def device_fn(x_in, d_y, w_q, w_k, w_v, w_o):
        rows, d_model = x_in.shape
        q_heads, head = w_q.shape[1], w_q.shape[2]
        kv_heads = w_k.shape[1]
        seq = rows * n_dev
        scale = head ** -0.5
        wide = q_heads // n_dev * head
        tile_w = kv_heads * head
        n_chunk = d_model // D_CHUNK
        wo_flat = w_o.reshape(q_heads * head, d_model)
        params = functools.partial(pltpu.CompilerParams, vmem_limit_bytes=VMEM_LIMIT)
        tri = (seq // BQ) * (seq // BQ + 1) // 2 * BQ
        return pl.pallas_call(
            functools.partial(fused_kernel, n_dev, scale),
            out_shape=(jax.ShapeDtypeStruct((rows, d_model), BF16),
                       jax.ShapeDtypeStruct((3 * n_chunk, D_CHUNK, tile_w), BF16)),
            in_specs=[vmem_spec, vmem_spec, any_spec, any_spec, any_spec, any_spec],
            out_specs=(vmem_spec, any_spec),
            scratch_shapes=[
                pltpu.VMEM((2 * rows, d_model), BF16),
                pltpu.VMEM((2 * rows, d_model), BF16),
                pltpu.VMEM((WO_DEPTH, wide, d_model), BF16),
                pltpu.VMEM((DEPTH, D_CHUNK, kv_heads, head), BF16),
                pltpu.VMEM((W2_DEPTH, D_CHUNK, tile_w), BF16),
                pltpu.VMEM((2 * rows, tile_w), F32),
                pltpu.VMEM((n_chip, 2 * rows, wide), BF16),
                pltpu.VMEM((2 * rows, tile_w), BF16),
                pltpu.VMEM((2, 2 * rows, tile_w), BF16),
                pltpu.VMEM((seq, wide), BF16),
                pltpu.VMEM((seq, wide), BF16),
                pltpu.VMEM((2, seq, head), BF16),
                pltpu.VMEM((head, seq), BF16),
                pltpu.VMEM((head, seq), BF16),
                pltpu.VMEM((wide // head, tri, BQ), BF16),
                pltpu.VMEM((wide // head, head, seq), BF16),
                pltpu.VMEM((seq, wide), BF16),
                pltpu.VMEM((2, seq, head), F32),
                pltpu.VMEM((2, 2 * rows, tile_w), BF16),
                pltpu.VMEM((2 * rows, tile_w), BF16),
                pltpu.VMEM((seq, head), F32),
                pltpu.VMEM((seq, head), BF16),
                pltpu.VMEM((3, tile_w, 2 * rows), BF16),
                pltpu.VMEM((n_chunk, D_CHUNK, 2 * rows), F32),
                pltpu.VMEM((n_chunk, D_CHUNK, rows), F32),
                dma((WO_DEPTH,)), dma((DEPTH,)), dma((W2_DEPTH,)), dma((2, 2)), dma((2, 2)),
                dma((n_chip, 2)), dma((n_chip, 2)), dma((n_chip, 2)), dma((n_chip, 2)),
                dma((n_chip, 2)), dma((n_chip, 2)), dma, dma,
                dma((seq // rows,)), dma((n_chip, 2)), dma((n_chip, 2)), dma((n_chip, 2)),
                dma((n_chunk,)), dma((n_chunk,)), dma, dma,
            ],
            compiler_params=params(collective_id=0, has_side_effects=True),
            name="fused",
        )(x_in, d_y, w_q, w_k, w_v, wo_flat)[0]

    return jax.shard_map(device_fn, mesh=mesh, in_specs=(row_spec, row_spec, P(), P(), P(), P()),
                         out_specs=row_spec, check_vma=False)
```

```python
import functools

import jax
import jax.numpy as jnp
from jax import lax
from jax.experimental import pallas as pl
from jax.experimental.pallas import tpu as pltpu
from jax.sharding import PartitionSpec as P

MESH = pl.DeviceIdType.MESH
BF16 = jnp.bfloat16
F32 = jnp.float32
CONTRACT_LAST = (((1,), (1,)), ((), ()))
DEPTH = 4
W2_DEPTH = 8
WO_DEPTH = 2
D_CHUNK = 512
BQ = 256
BK = 512
DO_FIRST = 4
VMEM_LIMIT = 62 * 2 ** 20


def place():
    me = lax.axis_index("cp")
    chip = me // 2
    core = me % 2
    return me, chip, core, me + 1 - 2 * core


def meet_group(n_dev):
    me = lax.axis_index("cp")
    barrier = pltpu.get_barrier_semaphore()

    def greet(step, carry):
        other = lax.rem(me + step, n_dev)
        pl.semaphore_signal(barrier, inc=1, device_id={"cp": other}, device_id_type=MESH)
        return carry

    lax.fori_loop(1, n_dev, greet, 0)
    pl.semaphore_wait(barrier, n_dev - 1)


def rcopy(src, dst, send_sem, recv_sem, dev):
    return pltpu.make_async_remote_copy(
        src_ref=src, dst_ref=dst, send_sem=send_sem, recv_sem=recv_sem,
        device_id={"cp": dev}, device_id_type=MESH)


def al(value, step):
    return pl.multiple_of(value, step)


def ship_start(is_me, src, dst, send_sem, recv_sem, dev):
    @pl.when(is_me)
    def _():
        pltpu.make_async_copy(src, dst, send_sem).start()

    @pl.when(jnp.logical_not(is_me))
    def _():
        rcopy(src, dst, send_sem, recv_sem, dev).start()


def ship_wait(is_me, src, dst, send_sem, recv_sem, dev):
    @pl.when(is_me)
    def _():
        pltpu.make_async_copy(src, dst, send_sem).wait()

    @pl.when(jnp.logical_not(is_me))
    def _():
        rcopy(src, dst, send_sem, recv_sem, dev).wait_send()


def fused_kernel(n_dev, scale, x_ref, dy_ref, wq, wk, wv, wo, dx_ref, w2_all,
                 xs, dys, wo_buf, w_buf, w2_buf, p_acc, st_do, st_kv, st_q,
                 q_all, do_all, kv_all, k_t, v_t, p_all, o_all, dq_st, dkv_acc,
                 dq_in, dkv_in, dkv_far, dkv_st, grads_t, acc, far,
                 wo_sem, w_sem, w2_sem, x_send, x_recv, do_send, do_recv,
                 kv_send, kv_recv, q_send, q_recv, rel_send, rel_recv,
                 dq_send, dq_recv, dkv_send, dkv_recv, far_send, far_recv, red_send, red_recv):
    me, chip, core, sib = place()
    n_chip = n_dev // 2
    rows, d_model = x_ref.shape
    seg = rows // 2
    seq, wide = q_all.shape
    head = kv_all.shape[2]
    heads = wide // head
    tile_w = p_acc.shape[1]
    n_chunk = d_model // D_CHUNK
    n_dest = n_dev // 2
    tile_heads = w_buf.shape[2]
    my_src_core = chip // (n_chip // 2)
    low_at = al(chip * rows, rows)
    high_at = al((2 * n_chip - 1 - chip) * rows, rows)
    n_block = seq // BQ
    per = BQ // rows
    to_log2 = scale * 1.4426950408889634

    def dest_of(n):
        spot, step = lax.rem(chip, 4), n // 2
        flip = 2 * lax.rem(spot // 2 + step // 2, 2) + lax.rem(spot + step, 2)
        return n_dest * core + 2 * flip + lax.rem(n, 2)

    def wo_copy(n):
        return pltpu.make_async_copy(
            wo.at[pl.ds(al(dest_of(n) * wide, wide), wide), :], wo_buf.at[lax.rem(n, WO_DEPTH)],
            wo_sem.at[lax.rem(n, WO_DEPTH)])

    def tile_of(t):
        return 2 * core + lax.rem(t + chip // 2, 2)

    def w_start(s):
        slot = lax.rem(s, DEPTH)
        part = lax.rem(s, n_chunk)
        d_rows = pl.ds(al(part * D_CHUNK, D_CHUNK), D_CHUNK)

        @pl.when((s < n_chunk) & (core == 0))
        def _():
            pltpu.make_async_copy(wk.at[d_rows], w_buf.at[slot], w_sem.at[slot]).start()

        @pl.when((s < n_chunk) & (core == 1))
        def _():
            pltpu.make_async_copy(wv.at[d_rows], w_buf.at[slot], w_sem.at[slot]).start()

        @pl.when((s >= n_chunk) & (s < 3 * n_chunk))
        def _():
            tile = tile_of(s // n_chunk - 1)
            pltpu.make_async_copy(
                wq.at[d_rows, pl.ds(al(tile * tile_heads, tile_heads), tile_heads), :],
                w_buf.at[slot], w_sem.at[slot]).start()

    def w_wait(s):
        slot = lax.rem(s, DEPTH)
        pltpu.make_async_copy(wk.at[pl.ds(0, D_CHUNK)], w_buf.at[slot], w_sem.at[slot]).wait()

    for n in range(WO_DEPTH - 1):
        wo_copy(jnp.int32(n)).start()
    for s in range(DEPTH - 1):
        w_start(jnp.int32(s))

    my_low = al(core * seg, seg)
    my_high = al(rows + (1 - core) * seg, seg)
    for ref, stack in ((dy_ref, dys), (x_ref, xs)):
        stack[pl.ds(my_low, seg), :] = ref[:seg, :]
        stack[pl.ds(my_high, seg), :] = ref[seg:, :]
    dkv_acc[...] = jnp.zeros_like(dkv_acc)
    meet_group(n_dev)
    swaps = []
    for k, (ref, stack) in enumerate(((dy_ref, dys), (x_ref, xs))):
        swaps.append(rcopy(ref.at[pl.ds(0, seg)], stack.at[pl.ds(my_low, seg)],
                           x_send.at[k, 0], x_recv.at[k, 0], sib))
        swaps.append(rcopy(ref.at[pl.ds(seg, seg)], stack.at[pl.ds(my_high, seg)],
                           x_send.at[k, 1], x_recv.at[k, 1], sib))
    swaps[0].start()
    swaps[1].start()
    swaps[0].wait()
    swaps[1].wait()
    swaps[2].start()
    swaps[3].start()

    def each(lo, hi, ship, act):
        def step(n, carry):
            ship(n, act)
            return carry
        lax.fori_loop(lo, hi, step, 0)

    def do_ship(n, act):
        dest = dest_of(n)
        for k, at in enumerate((low_at, high_at)):
            act(dest == me, st_do.at[n, pl.ds(k * rows, rows), :], do_all.at[pl.ds(at, rows), :],
                do_send.at[n, k], do_recv.at[chip, k], dest)

    def do_loop(lo, hi, send):
        def do_step(n, carry):
            @pl.when(n + WO_DEPTH - 1 < n_dest)
            def _():
                wo_copy(n + WO_DEPTH - 1).start()
            wo_copy(n).wait()

            if send:
                @pl.when(n > lo)
                def _():
                    do_ship(n - 1, ship_start)
            st_do[n] = lax.dot_general(dys[...], wo_buf[lax.rem(n, WO_DEPTH)], CONTRACT_LAST,
                                       preferred_element_type=F32).astype(BF16)
            return carry
        lax.fori_loop(lo, hi, do_step, 0)

    do_loop(0, DO_FIRST, True)
    swaps[2].wait()
    swaps[3].wait()

    def w2_copy(s):
        part = lax.rem(s, n_chunk)
        kind = s // n_chunk
        group = jnp.where(kind == 0, 0, 1 + lax.rem(kind - 1 + chip // 2, 2))
        slot = lax.rem(s, W2_DEPTH)
        return pltpu.make_async_copy(w2_buf.at[slot], w2_all.at[group * n_chunk + part], w2_sem.at[slot])

    def w_step(s, first):
        w_start(s + DEPTH - 1)
        w_wait(s)

        @pl.when(s >= 1)
        def _():
            w2_copy(s - 1).start()

        @pl.when(s >= W2_DEPTH)
        def _():
            w2_copy(s - W2_DEPTH).wait()
        part = lax.rem(s, n_chunk)
        w_tile = w_buf[lax.rem(s, DEPTH)].reshape(D_CHUNK, tile_w)
        w2_buf[lax.rem(s, W2_DEPTH)] = w_tile
        add = jnp.dot(xs[:, pl.ds(al(part * D_CHUNK, D_CHUNK), D_CHUNK)], w_tile,
                      preferred_element_type=F32)
        p_acc[...] = add if first else p_acc[...] + add

    def w_loop(lo, hi):
        def body(s, carry):
            w_step(s, False)
            return carry
        lax.fori_loop(lo, hi, body, 0)

    def kv_ship(n, act):
        dest_chip = lax.rem(n + chip, n_chip)
        dest = 2 * dest_chip + core
        lanes = pl.ds(al(dest_chip * head, head), head)
        for k, at in enumerate((low_at, high_at)):
            act(dest == me, st_kv.at[pl.ds(k * rows, rows), lanes], kv_all.at[core, pl.ds(at, rows), :],
                kv_send.at[dest_chip, k], kv_recv.at[chip, k], dest)

    def q_ship(n, act):
        t = n // 4
        dest = 4 * tile_of(t) + lax.rem(n + 2 * chip, 4)
        lanes = pl.ds(al(lax.rem(dest, 4) * wide, wide), wide)
        for k, at in enumerate((low_at, high_at)):
            act(dest == me, st_q.at[t, pl.ds(k * rows, rows), lanes], q_all.at[pl.ds(at, rows), :],
                q_send.at[n, k], q_recv.at[chip, k], dest)

    w_step(jnp.int32(0), True)
    do_ship(jnp.int32(DO_FIRST - 1), ship_start)
    w_loop(1, n_chunk)
    st_kv[...] = p_acc[...].astype(BF16)
    w_step(jnp.int32(n_chunk), True)
    each(0, n_chip, kv_ship, ship_start)
    w_loop(n_chunk + 1, 2 * n_chunk)
    st_q[0] = p_acc[...].astype(BF16)
    w_step(jnp.int32(2 * n_chunk), True)
    each(0, 4, q_ship, ship_start)
    w_loop(2 * n_chunk + 1, 3 * n_chunk)
    st_q[1] = p_acc[...].astype(BF16)
    w2_copy(jnp.int32(3 * n_chunk - 1)).start()

    def kv_arrive(src_chip, carry):
        @pl.when(src_chip != chip)
        def _():
            for k in range(2):
                rcopy(st_kv.at[pl.ds(0, rows), pl.ds(0, head)], kv_all.at[core, pl.ds(0, rows), :],
                      kv_send.at[0, k], kv_recv.at[src_chip, k], sib).wait_recv()
        return carry

    do_loop(DO_FIRST, DO_FIRST + 1, False)
    each(4, 8, q_ship, ship_start)
    do_loop(DO_FIRST + 1, n_dest, False)
    for k in range(W2_DEPTH):
        w2_copy(jnp.int32(3 * n_chunk - W2_DEPTH + k)).wait()
    lax.fori_loop(0, n_chip, kv_arrive, 0)
    each(0, n_chip, kv_ship, ship_wait)
    relay = rcopy(kv_all.at[core], kv_all.at[core], rel_send, rel_recv, sib)
    relay.start()
    rcopy(kv_all.at[core], kv_all.at[1 - core], rel_send, rel_recv, sib).wait_recv()
    relay.wait_send()
    k_t[...] = kv_all[0].T
    v_t[...] = kv_all[1].T
    each(0, 4, q_ship, ship_wait)

    def chunks_of(qb):
        cuts = list(range(0, qb * BQ, BK)) + [qb * BQ, (qb + 1) * BQ]
        return [slice(lo, hi) for lo, hi in zip(cuts[:-1], cuts[1:])]

    def s_at(ks):
        return slice(ks.start // BQ, ks.stop // BQ)

    def p_rows(qb, ks):
        base = BQ * (qb * (qb + 1) // 2)
        return slice(base + ks.start, base + ks.stop)

    def forward(qb):
        q_rows = slice(qb * BQ, (qb + 1) * BQ)
        q = [q_all[q_rows, h * head:(h + 1) * head] for h in range(heads)]
        chunks = chunks_of(qb)
        tops = [[] for _ in range(heads)]
        sums = [[] for _ in range(heads)]
        for ks in chunks:
            k_blk = kv_all[0, ks, :]
            for h in range(heads):
                s = lax.dot_general(k_blk, q[h], CONTRACT_LAST, preferred_element_type=F32)
                if ks.start == qb * BQ:
                    k_pos = lax.broadcasted_iota(jnp.int32, (BQ, BQ), 0)
                    q_pos = lax.broadcasted_iota(jnp.int32, (BQ, BQ), 1)
                    s = jnp.where(k_pos <= q_pos, s, -jnp.inf)
                top = jnp.max(s, axis=0, keepdims=True) * to_log2
                e = jnp.exp2(s * to_log2 - top)
                acc[s_at(ks), h * BQ:(h + 1) * BQ, :] = e.reshape(-1, BQ, BQ)
                tops[h].append(top)
                sums[h].append(jnp.sum(e, axis=0, keepdims=True))
        for h in range(heads):
            top = functools.reduce(jnp.maximum, tops[h])
            lift = [jnp.exp2(t - top) for t in tops[h]]
            inv = 1.0 / sum(a * b for a, b in zip(lift, sums[h]))
            o_t = None
            for ks, up in zip(chunks, lift):
                p = (acc[s_at(ks), h * BQ:(h + 1) * BQ, :].reshape(-1, BQ) * (up * inv)).astype(BF16)
                p_all[h, p_rows(qb, ks), :] = p
                part = jnp.dot(v_t[:, ks], p, preferred_element_type=F32)
                o_t = part if o_t is None else o_t + part
            o_all[h, :, q_rows] = o_t.astype(BF16)

    def backward(qb):
        q_rows = slice(qb * BQ, (qb + 1) * BQ)
        q = [q_all[q_rows, h * head:(h + 1) * head] for h in range(heads)]
        do = [do_all[q_rows, h * head:(h + 1) * head] for h in range(heads)]
        delta = [jnp.sum(do[h].astype(F32).T * o_all[h, :, q_rows].astype(F32), axis=0, keepdims=True)
                 for h in range(heads)]
        dq_t = [None] * heads
        for ks in chunks_of(qb):
            v_blk = kv_all[1, ks, :]
            dk = dv = None
            for h in range(heads):
                p = p_all[h, p_rows(qb, ks), :]
                dp = lax.dot_general(v_blk, do[h], CONTRACT_LAST, preferred_element_type=F32)
                ds = (p.astype(F32) * (dp - delta[h])).astype(BF16)
                part = jnp.dot(k_t[:, ks], ds, preferred_element_type=F32)
                dq_t[h] = part if dq_t[h] is None else dq_t[h] + part
                dk_h = jnp.dot(ds, q[h], preferred_element_type=F32)
                dv_h = jnp.dot(p, do[h], preferred_element_type=F32)
                dk = dk_h if dk is None else dk + dk_h
                dv = dv_h if dv is None else dv + dv_h
            dkv_acc[0, ks, :] += dk
            dkv_acc[1, ks, :] += dv
        for h in range(heads):
            dq_st[q_rows, h * head:(h + 1) * head] = (dq_t[h] * scale).T.astype(BF16)

    def block_at(step):
        side = lax.rem(lax.rem(chip, 4) // 2 + step // 4, 2)
        spot = lax.rem(step + lax.rem(chip, 2) + 2 * (chip // 4), 4)
        return jnp.where(spot < 2, 2 * spot + side, 11 - 2 * spot - side)

    def home_of(block):
        return jnp.where(block < n_chip, block, 2 * n_chip - 1 - block)

    def ahead(step, carry):
        qb = block_at(step)

        @pl.when(step == n_block // 2)
        def _():
            each(4, 6, q_ship, ship_wait)
            each(DO_FIRST, 6, do_ship, ship_start)

        @pl.when(step == n_block // 2 + 1)
        def _():
            each(6, 8, q_ship, ship_wait)
            each(6, n_dest, do_ship, ship_start)
        for i in range(per):
            block = qb * per + i
            home = home_of(block)

            @pl.when(2 * home + my_src_core != me)
            def _():
                rcopy(st_do.at[0, pl.ds(0, rows), :], q_all.at[pl.ds(0, rows), :],
                      q_send.at[0, 0], q_recv.at[home, block // n_chip], sib).wait_recv()
        for which in range(n_block):
            @pl.when(qb == which)
            def _():
                forward(which)
        return carry

    lax.fori_loop(0, n_block, ahead, 0)

    src_slot = lax.rem(me, n_dest)

    def dq_ship(block, act):
        k = block // n_chip
        dest = 2 * home_of(block) + my_src_core
        act(dest == me, dq_st.at[pl.ds(al(block * rows, rows), rows), :],
            dq_in.at[src_slot // 4, pl.ds(al(k * rows, rows), rows), pl.ds(al(lax.rem(src_slot, 4) * wide, wide), wide)],
            dq_send.at[block], dq_recv.at[src_slot, k], dest)

    def do_done(n, carry):
        @pl.when(dest_of(n) == me)
        def _():
            do_ship(n, ship_wait)
        return carry

    lax.fori_loop(0, n_dest, do_done, 0)

    def back(step, carry):
        qb = block_at(step)
        for i in range(per):
            block = qb * per + i
            home = home_of(block)

            @pl.when(2 * home + my_src_core != me)
            def _():
                rcopy(st_do.at[0, pl.ds(0, rows), :], do_all.at[pl.ds(0, rows), :],
                      do_send.at[0, 0], do_recv.at[home, block // n_chip], sib).wait_recv()
        for which in range(n_block):
            @pl.when(qb == which)
            def _():
                backward(which)
        for i in range(per):
            dq_ship(qb * per + i, ship_start)
        return carry

    lax.fori_loop(0, n_block, back, 0)
    swap = rcopy(dkv_acc.at[1 - core], dkv_far, red_send, red_recv, sib)
    swap.start()

    early = lax.rem(chip, 4) // 2
    n_pair = n_chunk // 2
    n_slot = W2_DEPTH // 2

    def stream_copy(u):
        turn = u // n_pair
        group = jnp.where(turn == 0, 1 + early, jnp.where(turn == 1, 2 - early, 0))
        part = group * n_chunk + 2 * lax.rem(u, n_pair)
        slot = lax.rem(u, n_slot)
        return pltpu.make_async_copy(w2_all.at[pl.ds(part, 2)], w2_buf.at[pl.ds(2 * slot, 2)], w2_sem.at[slot])

    for u in range(n_slot - 1):
        stream_copy(jnp.int32(u)).start()

    def do_sent(n, carry):
        @pl.when(dest_of(n) != me)
        def _():
            do_ship(n, ship_wait)
        return carry

    lax.fori_loop(0, n_dest, do_sent, 0)

    def dkv_ship(n, act):
        dest_chip = lax.rem(chip + n, n_chip)
        dest = 2 * dest_chip + core
        for k in range(2):
            block = dest_chip if k == 0 else 2 * n_chip - 1 - dest_chip
            act(dest == me, dkv_st.at[pl.ds(al(block * rows, rows), rows), :],
                dkv_in.at[pl.ds(k * rows, rows), pl.ds(al(chip * head, head), head)],
                dkv_send.at[n, k], dkv_recv.at[chip, k], dest)

    swap.wait()
    factor = jnp.where(core == 0, scale, 1.0).astype(F32)
    dkv_st[...] = ((dkv_acc[core] + dkv_far[...]) * factor).astype(BF16)
    each(0, n_chip, dkv_ship, ship_start)

    def dq_arrive(n, carry):
        src = lax.rem(4 * early + n, n_dest)

        @pl.when(n_dest * core + src != me)
        def _():
            for k in range(2):
                rcopy(dq_st.at[pl.ds(0, rows), :], dq_in.at[0, pl.ds(0, rows), pl.ds(0, wide)],
                      dq_send.at[0], dq_recv.at[src, k], sib).wait_recv()

        @pl.when(n_dest * core + src == me)
        def _():
            for k in range(2):
                dq_ship(jnp.where(k == 0, chip, 2 * n_chip - 1 - chip), ship_wait)
        return carry

    def by_token(x):
        return jnp.concatenate([x[:seg], x[3 * seg:], x[seg:3 * seg]], axis=0).T

    def matmul(group, u):
        @pl.when(u + n_slot - 1 < 3 * n_pair)
        def _():
            stream_copy(u + n_slot - 1).start()
        stream_copy(u).wait()
        pair = w2_buf[pl.ds(2 * lax.rem(u, n_slot), 2)].reshape(2 * D_CHUNK, tile_w)
        return jnp.dot(pair, grads_t[group], preferred_element_type=F32).reshape(2, D_CHUNK, 2 * rows)

    lax.fori_loop(0, n_dest // 2, dq_arrive, 0)
    grads_t[0] = by_token(dq_in[early])

    def early_pass(part, carry):
        acc[pl.ds(2 * part, 2)] = matmul(0, part)
        return carry

    lax.fori_loop(0, n_pair, early_pass, 0)
    lax.fori_loop(n_dest // 2, n_dest, dq_arrive, 0)
    grads_t[1] = by_token(dq_in[1 - early])

    def late_pass(part, carry):
        acc[pl.ds(2 * part, 2)] += matmul(1, n_pair + part)
        return carry

    lax.fori_loop(0, n_pair, late_pass, 0)

    def dq_sent(block, carry):
        @pl.when(2 * home_of(block) + my_src_core != me)
        def _():
            dq_ship(block, ship_wait)
        return carry

    lax.fori_loop(0, n_block * per, dq_sent, 0)
    each(0, n_chip, dkv_ship, ship_wait)

    def dkv_arrive(src_chip, carry):
        @pl.when(src_chip != chip)
        def _():
            for k in range(2):
                rcopy(dkv_st.at[pl.ds(0, rows), :], dkv_in.at[pl.ds(0, rows), pl.ds(0, head)],
                      dkv_send.at[0, k], dkv_recv.at[src_chip, k], sib).wait_recv()
        return carry

    lax.fori_loop(0, n_chip, dkv_arrive, 0)

    grads_t[2] = by_token(dkv_in[...])
    my_lanes = pl.ds(al(core * rows, rows), rows)
    sib_lanes = pl.ds(al((1 - core) * rows, rows), rows)

    def far_copy(part):
        two = pl.ds(2 * part, 2)
        return rcopy(acc.at[two, :, sib_lanes], far.at[two], far_send.at[part], far_recv.at[part], sib)

    def last_pass(part, carry):
        acc[pl.ds(2 * part, 2)] += matmul(2, 2 * n_pair + part)

        @pl.when(part > 0)
        def _():
            far_copy(part - 1).start()
        return carry

    lax.fori_loop(0, n_pair, last_pass, 0)
    far_copy(n_pair - 1).start()

    def finish(part, carry):
        far_copy(part).wait()
        for k in range(2):
            piece = 2 * part + k
            dx_ref[:, pl.ds(al(piece * D_CHUNK, D_CHUNK), D_CHUNK)] = (
                acc[piece, :, my_lanes] + far[piece]).astype(BF16).T
        return carry

    lax.fori_loop(0, n_pair, finish, 0)


def solution(mesh):
    n_dev = mesh.shape["cp"]
    n_chip = n_dev // 2
    row_spec = P(("dp", "cp"), None)
    any_spec = pl.BlockSpec(memory_space=pl.ANY)
    vmem_spec = pl.BlockSpec(memory_space=pltpu.VMEM)
    dma = pltpu.SemaphoreType.DMA

    def device_fn(x_in, d_y, w_q, w_k, w_v, w_o):
        rows, d_model = x_in.shape
        q_heads, head = w_q.shape[1], w_q.shape[2]
        kv_heads = w_k.shape[1]
        seq = rows * n_dev
        scale = head ** -0.5
        wide = q_heads // n_dev * head
        tile_w = kv_heads * head
        n_chunk = d_model // D_CHUNK
        wo_flat = w_o.reshape(q_heads * head, d_model)
        params = functools.partial(pltpu.CompilerParams, vmem_limit_bytes=VMEM_LIMIT)
        tri = (seq // BQ) * (seq // BQ + 1) // 2 * BQ
        return pl.pallas_call(
            functools.partial(fused_kernel, n_dev, scale),
            out_shape=(jax.ShapeDtypeStruct((rows, d_model), BF16),
                       jax.ShapeDtypeStruct((3 * n_chunk, D_CHUNK, tile_w), BF16)),
            in_specs=[vmem_spec, vmem_spec, any_spec, any_spec, any_spec, any_spec],
            out_specs=(vmem_spec, any_spec),
            scratch_shapes=[
                pltpu.VMEM((2 * rows, d_model), BF16),
                pltpu.VMEM((2 * rows, d_model), BF16),
                pltpu.VMEM((WO_DEPTH, wide, d_model), BF16),
                pltpu.VMEM((DEPTH, D_CHUNK, kv_heads, head), BF16),
                pltpu.VMEM((W2_DEPTH, D_CHUNK, tile_w), BF16),
                pltpu.VMEM((2 * rows, tile_w), F32),
                pltpu.VMEM((n_chip, 2 * rows, wide), BF16),
                pltpu.VMEM((2 * rows, tile_w), BF16),
                pltpu.VMEM((2, 2 * rows, tile_w), BF16),
                pltpu.VMEM((seq, wide), BF16),
                pltpu.VMEM((seq, wide), BF16),
                pltpu.VMEM((2, seq, head), BF16),
                pltpu.VMEM((head, seq), BF16),
                pltpu.VMEM((head, seq), BF16),
                pltpu.VMEM((wide // head, tri, BQ), BF16),
                pltpu.VMEM((wide // head, head, seq), BF16),
                pltpu.VMEM((seq, wide), BF16),
                pltpu.VMEM((2, seq, head), F32),
                pltpu.VMEM((2, 2 * rows, tile_w), BF16),
                pltpu.VMEM((2 * rows, tile_w), BF16),
                pltpu.VMEM((seq, head), F32),
                pltpu.VMEM((seq, head), BF16),
                pltpu.VMEM((3, tile_w, 2 * rows), BF16),
                pltpu.VMEM((n_chunk, D_CHUNK, 2 * rows), F32),
                pltpu.VMEM((n_chunk, D_CHUNK, rows), F32),
                dma((WO_DEPTH,)), dma((DEPTH,)), dma((W2_DEPTH,)), dma((2, 2)), dma((2, 2)),
                dma((n_chip, 2)), dma((n_chip, 2)), dma((n_chip, 2)), dma((n_chip, 2)),
                dma((n_chip, 2)), dma((n_chip, 2)), dma, dma,
                dma((seq // rows,)), dma((n_chip, 2)), dma((n_chip, 2)), dma((n_chip, 2)),
                dma((n_chunk,)), dma((n_chunk,)), dma, dma,
            ],
            compiler_params=params(collective_id=0, has_side_effects=True),
            name="fused",
        )(x_in, d_y, w_q, w_k, w_v, wo_flat)[0]

    return jax.shard_map(device_fn, mesh=mesh, in_specs=(row_spec, row_spec, P(), P(), P(), P()),
                         out_specs=row_spec, check_vma=False)
```

```python
import functools

import jax
import jax.numpy as jnp
from jax import lax
from jax.experimental import pallas as pl
from jax.experimental.pallas import tpu as pltpu
from jax.sharding import PartitionSpec as P

MESH = pl.DeviceIdType.MESH
BF16 = jnp.bfloat16
F32 = jnp.float32
CONTRACT_LAST = (((1,), (1,)), ((), ()))
DEPTH = 4
W2_DEPTH = 8
WO_DEPTH = 2
D_CHUNK = 512
BQ = 256
BK = 512
DO_FIRST = 4
VMEM_LIMIT = 62 * 2 ** 20


def place():
    me = lax.axis_index("cp")
    chip = me // 2
    core = me % 2
    return me, chip, core, me + 1 - 2 * core


def meet_group(n_dev):
    me = lax.axis_index("cp")
    barrier = pltpu.get_barrier_semaphore()

    def greet(step, carry):
        other = lax.rem(me + step, n_dev)
        pl.semaphore_signal(barrier, inc=1, device_id={"cp": other}, device_id_type=MESH)
        return carry

    lax.fori_loop(1, n_dev, greet, 0)
    pl.semaphore_wait(barrier, n_dev - 1)


def rcopy(src, dst, send_sem, recv_sem, dev):
    return pltpu.make_async_remote_copy(
        src_ref=src, dst_ref=dst, send_sem=send_sem, recv_sem=recv_sem,
        device_id={"cp": dev}, device_id_type=MESH)


def al(value, step):
    return pl.multiple_of(value, step)


def ship_start(is_me, src, dst, send_sem, recv_sem, dev):
    @pl.when(is_me)
    def _():
        pltpu.make_async_copy(src, dst, send_sem).start()

    @pl.when(jnp.logical_not(is_me))
    def _():
        rcopy(src, dst, send_sem, recv_sem, dev).start()


def ship_wait(is_me, src, dst, send_sem, recv_sem, dev):
    @pl.when(is_me)
    def _():
        pltpu.make_async_copy(src, dst, send_sem).wait()

    @pl.when(jnp.logical_not(is_me))
    def _():
        rcopy(src, dst, send_sem, recv_sem, dev).wait_send()


def fused_kernel(n_dev, scale, x_ref, dy_ref, wq, wk, wv, wo, dx_ref, w2_all,
                 xs, dys, wo_buf, w_buf, w2_buf, p_acc, st_do, st_kv, st_q,
                 q_all, do_all, kv_all, k_t, v_t, p_all, o_all, dq_st, dkv_acc,
                 dq_in, dkv_in, dkv_far, dkv_st, grads_t, acc, far,
                 wo_sem, w_sem, w2_sem, x_send, x_recv, do_send, do_recv,
                 kv_send, kv_recv, q_send, q_recv, rel_send, rel_recv,
                 dq_send, dq_recv, dkv_send, dkv_recv, far_send, far_recv, red_send, red_recv):
    me, chip, core, sib = place()
    n_chip = n_dev // 2
    rows, d_model = x_ref.shape
    seg = rows // 2
    seq, wide = q_all.shape
    head = kv_all.shape[2]
    heads = wide // head
    tile_w = p_acc.shape[1]
    n_chunk = d_model // D_CHUNK
    n_dest = n_dev // 2
    tile_heads = w_buf.shape[2]
    my_src_core = chip // (n_chip // 2)
    low_at = al(chip * rows, rows)
    high_at = al((2 * n_chip - 1 - chip) * rows, rows)
    n_block = seq // BQ
    per = BQ // rows
    to_log2 = scale * 1.4426950408889634

    def dest_of(n):
        spot, step = lax.rem(chip, 4), jnp.where(n < 4, 1 - n // 2, n // 2)
        flip = 2 * lax.rem(spot // 2 + step // 2, 2) + lax.rem(spot + step, 2)
        return n_dest * core + 2 * flip + lax.rem(n, 2)

    def wo_copy(n):
        return pltpu.make_async_copy(
            wo.at[pl.ds(al(dest_of(n) * wide, wide), wide), :], wo_buf.at[lax.rem(n, WO_DEPTH)],
            wo_sem.at[lax.rem(n, WO_DEPTH)])

    def tile_of(t):
        return 2 * core + lax.rem(t + chip // 2, 2)

    def w_start(s):
        slot = lax.rem(s, DEPTH)
        part = lax.rem(s, n_chunk)
        d_rows = pl.ds(al(part * D_CHUNK, D_CHUNK), D_CHUNK)

        @pl.when((s < n_chunk) & (core == 0))
        def _():
            pltpu.make_async_copy(wk.at[d_rows], w_buf.at[slot], w_sem.at[slot]).start()

        @pl.when((s < n_chunk) & (core == 1))
        def _():
            pltpu.make_async_copy(wv.at[d_rows], w_buf.at[slot], w_sem.at[slot]).start()

        @pl.when((s >= n_chunk) & (s < 3 * n_chunk))
        def _():
            tile = tile_of(s // n_chunk - 1)
            pltpu.make_async_copy(
                wq.at[d_rows, pl.ds(al(tile * tile_heads, tile_heads), tile_heads), :],
                w_buf.at[slot], w_sem.at[slot]).start()

    def w_wait(s):
        slot = lax.rem(s, DEPTH)
        pltpu.make_async_copy(wk.at[pl.ds(0, D_CHUNK)], w_buf.at[slot], w_sem.at[slot]).wait()

    for n in range(WO_DEPTH - 1):
        wo_copy(jnp.int32(n)).start()
    for s in range(DEPTH - 1):
        w_start(jnp.int32(s))

    my_low = al(core * seg, seg)
    my_high = al(rows + (1 - core) * seg, seg)
    for ref, stack in ((dy_ref, dys), (x_ref, xs)):
        stack[pl.ds(my_low, seg), :] = ref[:seg, :]
        stack[pl.ds(my_high, seg), :] = ref[seg:, :]
    dkv_acc[...] = jnp.zeros_like(dkv_acc)
    meet_group(n_dev)
    swaps = []
    for k, (ref, stack) in enumerate(((dy_ref, dys), (x_ref, xs))):
        swaps.append(rcopy(ref.at[pl.ds(0, seg)], stack.at[pl.ds(my_low, seg)],
                           x_send.at[k, 0], x_recv.at[k, 0], sib))
        swaps.append(rcopy(ref.at[pl.ds(seg, seg)], stack.at[pl.ds(my_high, seg)],
                           x_send.at[k, 1], x_recv.at[k, 1], sib))
    swaps[0].start()
    swaps[1].start()
    swaps[0].wait()
    swaps[1].wait()
    swaps[2].start()
    swaps[3].start()

    def each(lo, hi, ship, act):
        def step(n, carry):
            ship(n, act)
            return carry
        lax.fori_loop(lo, hi, step, 0)

    def do_ship(n, act):
        dest = dest_of(n)
        for k, at in enumerate((low_at, high_at)):
            act(dest == me, st_do.at[n, pl.ds(k * rows, rows), :], do_all.at[pl.ds(at, rows), :],
                do_send.at[n, k], do_recv.at[chip, k], dest)

    def do_loop(lo, hi, send):
        def do_step(n, carry):
            @pl.when(n + WO_DEPTH - 1 < n_dest)
            def _():
                wo_copy(n + WO_DEPTH - 1).start()
            wo_copy(n).wait()

            if send:
                @pl.when(n > lo)
                def _():
                    do_ship(n - 1, ship_start)
            st_do[n] = lax.dot_general(dys[...], wo_buf[lax.rem(n, WO_DEPTH)], CONTRACT_LAST,
                                       preferred_element_type=F32).astype(BF16)
            return carry
        lax.fori_loop(lo, hi, do_step, 0)

    do_loop(0, DO_FIRST, True)
    swaps[2].wait()
    swaps[3].wait()

    def w2_copy(s):
        part = lax.rem(s, n_chunk)
        kind = s // n_chunk
        group = jnp.where(kind == 0, 0, 1 + lax.rem(kind - 1 + chip // 2, 2))
        slot = lax.rem(s, W2_DEPTH)
        return pltpu.make_async_copy(w2_buf.at[slot], w2_all.at[group * n_chunk + part], w2_sem.at[slot])

    def w_step(s, first):
        w_start(s + DEPTH - 1)
        w_wait(s)

        @pl.when(s >= 1)
        def _():
            w2_copy(s - 1).start()

        @pl.when(s >= W2_DEPTH)
        def _():
            w2_copy(s - W2_DEPTH).wait()
        part = lax.rem(s, n_chunk)
        w_tile = w_buf[lax.rem(s, DEPTH)].reshape(D_CHUNK, tile_w)
        w2_buf[lax.rem(s, W2_DEPTH)] = w_tile
        add = jnp.dot(xs[:, pl.ds(al(part * D_CHUNK, D_CHUNK), D_CHUNK)], w_tile,
                      preferred_element_type=F32)
        p_acc[...] = add if first else p_acc[...] + add

    def w_loop(lo, hi):
        def body(s, carry):
            w_step(s, False)
            return carry
        lax.fori_loop(lo, hi, body, 0)

    def kv_ship(n, act):
        dest_chip = lax.rem(n + 1 + chip, n_chip)
        dest = 2 * dest_chip + core
        lanes = pl.ds(al(dest_chip * head, head), head)
        for k, at in enumerate((low_at, high_at)):
            act(dest == me, st_kv.at[pl.ds(k * rows, rows), lanes], kv_all.at[core, pl.ds(at, rows), :],
                kv_send.at[dest_chip, k], kv_recv.at[chip, k], dest)

    def q_ship(n, act):
        t = n // 4
        dest = 4 * tile_of(t) + lax.rem(n + 2 + 2 * chip, 4)
        lanes = pl.ds(al(lax.rem(dest, 4) * wide, wide), wide)
        for k, at in enumerate((low_at, high_at)):
            act(dest == me, st_q.at[t, pl.ds(k * rows, rows), lanes], q_all.at[pl.ds(at, rows), :],
                q_send.at[n, k], q_recv.at[chip, k], dest)

    w_step(jnp.int32(0), True)
    do_ship(jnp.int32(DO_FIRST - 1), ship_start)
    w_loop(1, n_chunk)
    st_kv[...] = p_acc[...].astype(BF16)
    w_step(jnp.int32(n_chunk), True)
    each(0, n_chip, kv_ship, ship_start)
    w_loop(n_chunk + 1, 2 * n_chunk)
    st_q[0] = p_acc[...].astype(BF16)
    w_step(jnp.int32(2 * n_chunk), True)
    each(0, 4, q_ship, ship_start)
    w_loop(2 * n_chunk + 1, 3 * n_chunk)
    st_q[1] = p_acc[...].astype(BF16)
    w2_copy(jnp.int32(3 * n_chunk - 1)).start()

    def kv_arrive(src_chip, carry):
        @pl.when(src_chip != chip)
        def _():
            for k in range(2):
                rcopy(st_kv.at[pl.ds(0, rows), pl.ds(0, head)], kv_all.at[core, pl.ds(0, rows), :],
                      kv_send.at[0, k], kv_recv.at[src_chip, k], sib).wait_recv()
        return carry

    do_loop(DO_FIRST, DO_FIRST + 1, False)
    each(4, 8, q_ship, ship_start)
    do_loop(DO_FIRST + 1, n_dest, False)
    for k in range(W2_DEPTH):
        w2_copy(jnp.int32(3 * n_chunk - W2_DEPTH + k)).wait()
    lax.fori_loop(0, n_chip, kv_arrive, 0)
    each(0, n_chip, kv_ship, ship_wait)
    relay = rcopy(kv_all.at[core], kv_all.at[core], rel_send, rel_recv, sib)
    relay.start()
    rcopy(kv_all.at[core], kv_all.at[1 - core], rel_send, rel_recv, sib).wait_recv()
    relay.wait_send()
    k_t[...] = kv_all[0].T
    v_t[...] = kv_all[1].T
    each(0, 4, q_ship, ship_wait)

    def chunks_of(qb):
        cuts = list(range(0, qb * BQ, BK)) + [qb * BQ, (qb + 1) * BQ]
        return [slice(lo, hi) for lo, hi in zip(cuts[:-1], cuts[1:])]

    def s_at(ks):
        return slice(ks.start // BQ, ks.stop // BQ)

    def p_rows(qb, ks):
        base = BQ * (qb * (qb + 1) // 2)
        return slice(base + ks.start, base + ks.stop)

    def forward(qb):
        q_rows = slice(qb * BQ, (qb + 1) * BQ)
        q = [q_all[q_rows, h * head:(h + 1) * head] for h in range(heads)]
        chunks = chunks_of(qb)
        tops = [[] for _ in range(heads)]
        sums = [[] for _ in range(heads)]
        for ks in chunks:
            k_blk = kv_all[0, ks, :]
            for h in range(heads):
                s = lax.dot_general(k_blk, q[h], CONTRACT_LAST, preferred_element_type=F32)
                if ks.start == qb * BQ:
                    k_pos = lax.broadcasted_iota(jnp.int32, (BQ, BQ), 0)
                    q_pos = lax.broadcasted_iota(jnp.int32, (BQ, BQ), 1)
                    s = jnp.where(k_pos <= q_pos, s, -jnp.inf)
                top = jnp.max(s, axis=0, keepdims=True) * to_log2
                e = jnp.exp2(s * to_log2 - top)
                acc[s_at(ks), h * BQ:(h + 1) * BQ, :] = e.reshape(-1, BQ, BQ)
                tops[h].append(top)
                sums[h].append(jnp.sum(e, axis=0, keepdims=True))
        for h in range(heads):
            top = functools.reduce(jnp.maximum, tops[h])
            lift = [jnp.exp2(t - top) for t in tops[h]]
            inv = 1.0 / sum(a * b for a, b in zip(lift, sums[h]))
            o_t = None
            for ks, up in zip(chunks, lift):
                p = (acc[s_at(ks), h * BQ:(h + 1) * BQ, :].reshape(-1, BQ) * (up * inv)).astype(BF16)
                p_all[h, p_rows(qb, ks), :] = p
                part = jnp.dot(v_t[:, ks], p, preferred_element_type=F32)
                o_t = part if o_t is None else o_t + part
            o_all[h, :, q_rows] = o_t.astype(BF16)

    def backward(qb):
        q_rows = slice(qb * BQ, (qb + 1) * BQ)
        q = [q_all[q_rows, h * head:(h + 1) * head] for h in range(heads)]
        do = [do_all[q_rows, h * head:(h + 1) * head] for h in range(heads)]
        delta = [jnp.sum(do[h].astype(F32).T * o_all[h, :, q_rows].astype(F32), axis=0, keepdims=True)
                 for h in range(heads)]
        dq_t = [None] * heads
        for ks in chunks_of(qb):
            v_blk = kv_all[1, ks, :]
            dk = dv = None
            for h in range(heads):
                p = p_all[h, p_rows(qb, ks), :]
                dp = lax.dot_general(v_blk, do[h], CONTRACT_LAST, preferred_element_type=F32)
                ds = (p.astype(F32) * (dp - delta[h])).astype(BF16)
                part = jnp.dot(k_t[:, ks], ds, preferred_element_type=F32)
                dq_t[h] = part if dq_t[h] is None else dq_t[h] + part
                dk_h = jnp.dot(ds, q[h], preferred_element_type=F32)
                dv_h = jnp.dot(p, do[h], preferred_element_type=F32)
                dk = dk_h if dk is None else dk + dk_h
                dv = dv_h if dv is None else dv + dv_h
            dkv_acc[0, ks, :] += dk
            dkv_acc[1, ks, :] += dv
        for h in range(heads):
            dq_st[q_rows, h * head:(h + 1) * head] = (dq_t[h] * scale).T.astype(BF16)

    def block_at(step):
        side = lax.rem(lax.rem(chip, 4) // 2 + step // 4, 2)
        spot = lax.rem(step + lax.rem(chip, 2) + 2 * (chip // 4), 4)
        return jnp.where(spot < 2, 2 * spot + side, 11 - 2 * spot - side)

    def home_of(block):
        return jnp.where(block < n_chip, block, 2 * n_chip - 1 - block)

    def ahead(step, carry):
        qb = block_at(step)

        @pl.when(step == n_block // 2)
        def _():
            each(4, 6, q_ship, ship_wait)
            each(DO_FIRST, 6, do_ship, ship_start)

        @pl.when(step == n_block // 2 + 1)
        def _():
            each(6, 8, q_ship, ship_wait)
            each(6, n_dest, do_ship, ship_start)
        for i in range(per):
            block = qb * per + i
            home = home_of(block)

            @pl.when(2 * home + my_src_core != me)
            def _():
                rcopy(st_do.at[0, pl.ds(0, rows), :], q_all.at[pl.ds(0, rows), :],
                      q_send.at[0, 0], q_recv.at[home, block // n_chip], sib).wait_recv()
        for which in range(n_block):
            @pl.when(qb == which)
            def _():
                forward(which)
        return carry

    lax.fori_loop(0, n_block, ahead, 0)

    src_slot = lax.rem(me, n_dest)

    def dq_ship(block, act):
        k = block // n_chip
        dest = 2 * home_of(block) + my_src_core
        act(dest == me, dq_st.at[pl.ds(al(block * rows, rows), rows), :],
            dq_in.at[src_slot // 4, pl.ds(al(k * rows, rows), rows), pl.ds(al(lax.rem(src_slot, 4) * wide, wide), wide)],
            dq_send.at[block], dq_recv.at[src_slot, k], dest)

    def do_done(n, carry):
        @pl.when(dest_of(n) == me)
        def _():
            do_ship(n, ship_wait)
        return carry

    lax.fori_loop(0, n_dest, do_done, 0)

    def back(step, carry):
        qb = block_at(step)
        for i in range(per):
            block = qb * per + i
            home = home_of(block)

            @pl.when(2 * home + my_src_core != me)
            def _():
                rcopy(st_do.at[0, pl.ds(0, rows), :], do_all.at[pl.ds(0, rows), :],
                      do_send.at[0, 0], do_recv.at[home, block // n_chip], sib).wait_recv()
        for which in range(n_block):
            @pl.when(qb == which)
            def _():
                backward(which)
        for i in range(per):
            dq_ship(qb * per + i, ship_start)
        return carry

    lax.fori_loop(0, n_block, back, 0)
    swap = rcopy(dkv_acc.at[1 - core], dkv_far, red_send, red_recv, sib)
    swap.start()

    early = lax.rem(chip, 4) // 2
    n_pair = n_chunk // 2
    n_slot = W2_DEPTH // 2

    def stream_copy(u):
        turn = u // n_pair
        group = jnp.where(turn == 0, 1 + early, jnp.where(turn == 1, 2 - early, 0))
        part = group * n_chunk + 2 * lax.rem(u, n_pair)
        slot = lax.rem(u, n_slot)
        return pltpu.make_async_copy(w2_all.at[pl.ds(part, 2)], w2_buf.at[pl.ds(2 * slot, 2)], w2_sem.at[slot])

    for u in range(n_slot - 1):
        stream_copy(jnp.int32(u)).start()

    def do_sent(n, carry):
        @pl.when(dest_of(n) != me)
        def _():
            do_ship(n, ship_wait)
        return carry

    lax.fori_loop(0, n_dest, do_sent, 0)

    def dkv_ship(n, act):
        dest_chip = lax.rem(chip + n, n_chip)
        dest = 2 * dest_chip + core
        for k in range(2):
            block = dest_chip if k == 0 else 2 * n_chip - 1 - dest_chip
            act(dest == me, dkv_st.at[pl.ds(al(block * rows, rows), rows), :],
                dkv_in.at[pl.ds(k * rows, rows), pl.ds(al(chip * head, head), head)],
                dkv_send.at[n, k], dkv_recv.at[chip, k], dest)

    swap.wait()
    factor = jnp.where(core == 0, scale, 1.0).astype(F32)
    dkv_st[...] = ((dkv_acc[core] + dkv_far[...]) * factor).astype(BF16)
    each(0, n_chip, dkv_ship, ship_start)

    def dq_arrive(n, carry):
        src = lax.rem(4 * early + n, n_dest)

        @pl.when(n_dest * core + src != me)
        def _():
            for k in range(2):
                rcopy(dq_st.at[pl.ds(0, rows), :], dq_in.at[0, pl.ds(0, rows), pl.ds(0, wide)],
                      dq_send.at[0], dq_recv.at[src, k], sib).wait_recv()

        @pl.when(n_dest * core + src == me)
        def _():
            for k in range(2):
                dq_ship(jnp.where(k == 0, chip, 2 * n_chip - 1 - chip), ship_wait)
        return carry

    def by_token(x):
        return jnp.concatenate([x[:seg], x[3 * seg:], x[seg:3 * seg]], axis=0).T

    def matmul(group, u):
        @pl.when(u + n_slot - 1 < 3 * n_pair)
        def _():
            stream_copy(u + n_slot - 1).start()
        stream_copy(u).wait()
        pair = w2_buf[pl.ds(2 * lax.rem(u, n_slot), 2)].reshape(2 * D_CHUNK, tile_w)
        return jnp.dot(pair, grads_t[group], preferred_element_type=F32).reshape(2, D_CHUNK, 2 * rows)

    lax.fori_loop(0, n_dest // 2, dq_arrive, 0)
    grads_t[0] = by_token(dq_in[early])

    def early_pass(part, carry):
        acc[pl.ds(2 * part, 2)] = matmul(0, part)
        return carry

    lax.fori_loop(0, n_pair, early_pass, 0)
    lax.fori_loop(n_dest // 2, n_dest, dq_arrive, 0)
    grads_t[1] = by_token(dq_in[1 - early])

    def late_pass(part, carry):
        acc[pl.ds(2 * part, 2)] += matmul(1, n_pair + part)
        return carry

    lax.fori_loop(0, n_pair, late_pass, 0)

    def dq_sent(block, carry):
        @pl.when(2 * home_of(block) + my_src_core != me)
        def _():
            dq_ship(block, ship_wait)
        return carry

    lax.fori_loop(0, n_block * per, dq_sent, 0)
    each(0, n_chip, dkv_ship, ship_wait)

    def dkv_arrive(src_chip, carry):
        @pl.when(src_chip != chip)
        def _():
            for k in range(2):
                rcopy(dkv_st.at[pl.ds(0, rows), :], dkv_in.at[pl.ds(0, rows), pl.ds(0, head)],
                      dkv_send.at[0, k], dkv_recv.at[src_chip, k], sib).wait_recv()
        return carry

    lax.fori_loop(0, n_chip, dkv_arrive, 0)

    grads_t[2] = by_token(dkv_in[...])
    my_lanes = pl.ds(al(core * rows, rows), rows)
    sib_lanes = pl.ds(al((1 - core) * rows, rows), rows)

    def far_copy(part):
        two = pl.ds(2 * part, 2)
        return rcopy(acc.at[two, :, sib_lanes], far.at[two], far_send.at[part], far_recv.at[part], sib)

    def finish(part):
        far_copy(part).wait()
        for k in range(2):
            piece = 2 * part + k
            dx_ref[:, pl.ds(al(piece * D_CHUNK, D_CHUNK), D_CHUNK)] = (
                acc[piece, :, my_lanes] + far[piece]).astype(BF16).T

    def last_pass(part, carry):
        acc[pl.ds(2 * part, 2)] += matmul(2, 2 * n_pair + part)

        @pl.when(part > 1)
        def _():
            finish(part - 2)
        far_copy(part).start()
        return carry

    lax.fori_loop(0, n_pair, last_pass, 0)
    finish(n_pair - 2)
    finish(n_pair - 1)


def solution(mesh):
    n_dev = mesh.shape["cp"]
    n_chip = n_dev // 2
    row_spec = P(("dp", "cp"), None)
    any_spec = pl.BlockSpec(memory_space=pl.ANY)
    vmem_spec = pl.BlockSpec(memory_space=pltpu.VMEM)
    dma = pltpu.SemaphoreType.DMA

    def device_fn(x_in, d_y, w_q, w_k, w_v, w_o):
        rows, d_model = x_in.shape
        q_heads, head = w_q.shape[1], w_q.shape[2]
        kv_heads = w_k.shape[1]
        seq = rows * n_dev
        scale = head ** -0.5
        wide = q_heads // n_dev * head
        tile_w = kv_heads * head
        n_chunk = d_model // D_CHUNK
        wo_flat = w_o.reshape(q_heads * head, d_model)
        params = functools.partial(pltpu.CompilerParams, vmem_limit_bytes=VMEM_LIMIT)
        tri = (seq // BQ) * (seq // BQ + 1) // 2 * BQ
        return pl.pallas_call(
            functools.partial(fused_kernel, n_dev, scale),
            out_shape=(jax.ShapeDtypeStruct((rows, d_model), BF16),
                       jax.ShapeDtypeStruct((3 * n_chunk, D_CHUNK, tile_w), BF16)),
            in_specs=[vmem_spec, vmem_spec, any_spec, any_spec, any_spec, any_spec],
            out_specs=(vmem_spec, any_spec),
            scratch_shapes=[
                pltpu.VMEM((2 * rows, d_model), BF16),
                pltpu.VMEM((2 * rows, d_model), BF16),
                pltpu.VMEM((WO_DEPTH, wide, d_model), BF16),
                pltpu.VMEM((DEPTH, D_CHUNK, kv_heads, head), BF16),
                pltpu.VMEM((W2_DEPTH, D_CHUNK, tile_w), BF16),
                pltpu.VMEM((2 * rows, tile_w), F32),
                pltpu.VMEM((n_chip, 2 * rows, wide), BF16),
                pltpu.VMEM((2 * rows, tile_w), BF16),
                pltpu.VMEM((2, 2 * rows, tile_w), BF16),
                pltpu.VMEM((seq, wide), BF16),
                pltpu.VMEM((seq, wide), BF16),
                pltpu.VMEM((2, seq, head), BF16),
                pltpu.VMEM((head, seq), BF16),
                pltpu.VMEM((head, seq), BF16),
                pltpu.VMEM((wide // head, tri, BQ), BF16),
                pltpu.VMEM((wide // head, head, seq), BF16),
                pltpu.VMEM((seq, wide), BF16),
                pltpu.VMEM((2, seq, head), F32),
                pltpu.VMEM((2, 2 * rows, tile_w), BF16),
                pltpu.VMEM((2 * rows, tile_w), BF16),
                pltpu.VMEM((seq, head), F32),
                pltpu.VMEM((seq, head), BF16),
                pltpu.VMEM((3, tile_w, 2 * rows), BF16),
                pltpu.VMEM((n_chunk, D_CHUNK, 2 * rows), F32),
                pltpu.VMEM((n_chunk, D_CHUNK, rows), F32),
                dma((WO_DEPTH,)), dma((DEPTH,)), dma((W2_DEPTH,)), dma((2, 2)), dma((2, 2)),
                dma((n_chip, 2)), dma((n_chip, 2)), dma((n_chip, 2)), dma((n_chip, 2)),
                dma((n_chip, 2)), dma((n_chip, 2)), dma, dma,
                dma((seq // rows,)), dma((n_chip, 2)), dma((n_chip, 2)), dma((n_chip, 2)),
                dma((n_chunk,)), dma((n_chunk,)), dma, dma,
            ],
            compiler_params=params(collective_id=0, has_side_effects=True),
            name="fused",
        )(x_in, d_y, w_q, w_k, w_v, wo_flat)[0]

    return jax.shard_map(device_fn, mesh=mesh, in_specs=(row_spec, row_spec, P(), P(), P(), P()),
                         out_specs=row_spec, check_vma=False)
```
